512 devices in a mesh: gx: 8 (over y, core), gy: 16 (over z), gz: 4 (over x).
Axes of the slice: x: 4, y: 4, z: 16, core: 2. Of those that a mesh axis runs over, the one named last changes fastest.
Arguments:
- source_term: float32 [32, 32, 128, 512], P(None, 'gx', 'gy', 'gz'), may hold values from -16 to 16
- labels: int32 [32, 128, 512], P('gx', 'gy', 'gz'), may hold values from 0 to 5
- conductivity_table: float32 [6], replicated, may hold values from 0.05 to 1
- send_map: int32 [8, 16, 4, 256], P('gx', 'gy', 'gz'), may hold values from -1 to 4095, as said below
- owner_slots: int32 [65536], P(('gx', 'gy', 'gz')), may hold values from 0 to 255, as said below
- sensor_data: float32 [32, 128], replicated, may hold values from -6 to 6
Outputs:
- projections: float32 [3, 128, 65536], P(None, None, ('gx', 'gy', 'gz'))
- gram_blocks: float32 [6, 65536], P(None, ('gx', 'gy', 'gz'))
The draws below stay inside these ranges and needn't reach their ends.
Inputs may be any that keep to these rules, and one draw needn't show every extreme that they name: `send_map`: entries q * 2 to q * 2 + 1 of row (sx, sy, iz) hold, in their first slots, the brick-local voxels (i * 8 + j) * 128 + k of the positions that this brick sends to owner q = ix * 16 + iy of the same iz, and -1 in the others; no voxel appears twice in a row; some brick fills all 2 slots of some owner. `owner_slots`: the 128 entries of owner d = (ix * 16 + iy) * 4 + iz name, each once, exactly the slots src * 2 + slot that the bricks src = sx * 16 + sy with the same iz fill for it.
All inputs are finite; a program needn't handle non-finite values.
Results may differ from the reference program's by a relative error of at most 0.00012.
Values sent between devices are 32-bit elements; how exact they have to be, the bound alone decides.
A program may use at most 64 MiB of HBM per device.

```python
import math
import jax
import jax.numpy as jnp
from jax import lax

S = 32
TIMES = 128
NLAB = 6
CX = 4
CY = 8
CZ = 128
POS_OWN = 128
CAP = 2
NX = 32
NY = 128
NZ = 512
POSITIONS = 65536
N_GX = 8
N_GY = 16
N_GZ = 4


def draw_source_term(key, part):
    noise = jnp.clip(jax.random.normal(jax.random.fold_in(key, 11), (S, NX, NY, NZ), jnp.float32), -3.0, 3.0)
    xpos = jnp.arange(NX, dtype=jnp.float32)
    ramp = (0.5 + xpos / NX)[None, :, None, None]
    field = noise * ramp
    return jnp.clip(field, -16.0, 16.0)


def draw_labels(key, part):

    def radial(count):
        offsets = 2 * jnp.arange(count, dtype=jnp.int32) - (count - 1)
        return offsets * offsets * 64 // (count * count)
    radius = radial(NX)[:, None, None] + radial(NY)[None, :, None] + radial(NZ)[None, None, :]
    shell = jnp.minimum(radius * NLAB // 193, NLAB - 1)
    jumping = jax.random.randint(jax.random.fold_in(key, 21), (NX, NY, NZ), 0, 3)
    other = jax.random.randint(jax.random.fold_in(key, 22), (NX, NY, NZ), 0, NLAB)
    return jnp.where(jumping == 0, other, shell).astype(jnp.int32)


def position_plan(key):
    peers = N_GX * N_GY
    capacity = 2 * POS_OWN // peers
    cells = CX * CY * CZ
    order_keys = jax.random.split(jax.random.fold_in(key, 31), N_GZ)
    brick_order = jax.vmap(lambda one_key: jax.random.permutation(one_key, peers))(order_keys)
    level = jax.random.randint(jax.random.fold_in(key, 32), (N_GZ, peers // 2, 1), 0, capacity + 1)
    spread = capacity // 4
    jitter = jax.random.randint(jax.random.fold_in(key, 33), (N_GZ, peers // 2, peers), -spread, spread + 1)
    first = jnp.clip(level + jitter, 0, capacity)
    first = first.at[:, 0, 0].set(capacity)
    paired = jnp.stack([first, capacity - first], axis=2).reshape(N_GZ, peers, peers)
    ranking = jnp.argsort(brick_order, axis=1)
    counts = jnp.take_along_axis(paired, ranking[:, :, None], axis=1)
    starts = jnp.cumsum(counts, axis=2) - counts
    slot_range = jnp.arange(capacity, dtype=jnp.int32)
    voxel_keys = jax.random.split(jax.random.fold_in(key, 34), N_GZ * peers)
    voxel_order = jax.vmap(lambda one_key: jax.random.permutation(one_key, cells))(voxel_keys).reshape(N_GZ, peers, cells)
    wanted = (starts[:, :, :, None] + slot_range).reshape(N_GZ, peers, peers * capacity)
    valid = (slot_range < counts[:, :, :, None]).reshape(N_GZ, peers, peers * capacity)
    picked = jnp.take_along_axis(voxel_order, jnp.clip(wanted, 0, cells - 1), axis=2)
    sent = jnp.where(valid, picked, -1)
    send_map = jnp.transpose(sent, (1, 0, 2)).reshape(N_GX, N_GY, N_GZ, peers * capacity)
    arrived = (slot_range < jnp.transpose(counts, (0, 2, 1))[:, :, :, None]).reshape(N_GZ, peers, peers * capacity)
    score_keys = jax.random.split(jax.random.fold_in(key, 35), N_GZ * peers)
    scores = jax.vmap(lambda one_key: jax.random.permutation(one_key, peers * capacity))(score_keys).reshape(N_GZ, peers, peers * capacity)
    ranked = jnp.argsort(jnp.where(arrived, scores, scores + peers * capacity), axis=2)[:, :, :POS_OWN]
    owner_slots = jnp.transpose(ranked, (1, 0, 2)).reshape(-1)
    return (send_map.astype(jnp.int32), owner_slots.astype(jnp.int32))


def draw_send_map(key, part):
    return position_plan(key)[0]


def draw_owner_slots(key, part):
    return position_plan(key)[1]


def bell_draw(rng, shape, scale, limit, kind=jnp.bfloat16):
    drawn = jax.random.normal(rng, shape, jnp.float32) * scale
    return jnp.minimum(jnp.maximum(drawn, -limit), limit).astype(kind)


def setup_inputs(seed: int = 0) -> dict:
    key_list = jax.random.split(jax.random.key(seed), 7)
    source_term = draw_source_term(jax.random.fold_in(key_list[6], 71), 0)
    labels = draw_labels(jax.random.fold_in(key_list[6], 71), 0)
    conductivity_table = jnp.clip(jnp.exp(jax.random.uniform(key_list[2], (NLAB,), jnp.float32, math.log(0.05), math.log(1.0))), 0.05, 1.0)
    send_map = draw_send_map(jax.random.fold_in(key_list[6], 71), 0)
    owner_slots = draw_owner_slots(jax.random.fold_in(key_list[6], 71), 0)
    sensor_data = bell_draw(key_list[5], (S, TIMES), 1.0, 6.0, jnp.float32)
    return {"source_term": source_term, "labels": labels, "conductivity_table": conductivity_table, "send_map": send_map, "owner_slots": owner_slots, "sensor_data": sensor_data}


mass_term = 0.25


def tissue(shifted, table):
    conductivity = jnp.zeros(shifted.shape, table.dtype)
    for tissue_level in range(table.shape[0]):
        conductivity = conductivity + jnp.where(shifted == tissue_level + 1, table[tissue_level], 0.0)
    inside = (shifted > 0).astype(table.dtype)
    return conductivity, inside


def neighbour_slices(dim_index, offset):
    selection = [slice(1, -1), slice(1, -1), slice(1, -1)]
    selection[dim_index] = slice(2, None) if offset > 0 else slice(0, -2)
    return tuple(selection)


def stencil(padded, conductivity, inside):
    leading = (slice(None),) * (padded.ndim - 3)
    middle = (slice(1, -1), slice(1, -1), slice(1, -1))
    centre = padded[leading + middle]
    own_cond = conductivity[middle]
    own_in = inside[middle]
    accumulated = mass_term * centre
    for dim_index in range(3):
        for offset in (-1, 1):
            beside_all = neighbour_slices(dim_index, offset)
            weight = 0.5 * (own_cond + conductivity[beside_all]) * own_in * inside[beside_all]
            accumulated = accumulated + weight * (centre - padded[leading + beside_all])
    return accumulated


def gram_rows(leadfield):
    entry_pairs = ((0, 0), (1, 1), (2, 2), (0, 1), (0, 2), (1, 2))
    return jnp.stack([jnp.sum(leadfield[first] * leadfield[second], axis=0) for first, second in entry_pairs])


def solve_one(source_field, conductivity, inside):
    solution = jnp.zeros_like(source_field)
    residual = source_field
    direction = source_field
    current = jnp.sum(residual * residual)
    for turn_index in range(2):
        applied = stencil(jnp.pad(direction, 1), conductivity, inside)
        step_size = current / jnp.sum(direction * applied)
        solution = solution + step_size * direction
        residual = residual - step_size * applied
        if turn_index == 0:
            following = jnp.sum(residual * residual)
            direction = residual + (following / current) * direction
            current = following
    return solution


def reference(source_term, labels, conductivity_table, send_map, owner_slots, sensor_data):
    shifted = jnp.pad(labels + 1, 1)
    conductivity, inside = tissue(shifted, conductivity_table)
    positions = jnp.arange(POSITIONS, dtype=jnp.int32)
    device = positions // POS_OWN
    owner_x = device // (N_GY * N_GZ)
    owner_y = (device // N_GZ) % N_GY
    owner_z = device % N_GZ
    owner = owner_x * N_GY + owner_y
    source_peer = owner_slots // CAP
    slot_index = owner_slots % CAP
    source_x = source_peer // N_GY
    source_y = source_peer % N_GY
    voxel = send_map[source_x, source_y, owner_z, owner * CAP + slot_index]
    cell_x = source_x * CX + voxel // (CY * CZ) + 1
    cell_y = source_y * CY + (voxel // CZ) % CY + 1
    cell_z = owner_z * CZ + voxel % CZ + 1
    cond_here = conductivity[cell_x, cell_y, cell_z]

    def one_sensor(source_field):
        solution = solve_one(source_field, conductivity, inside)
        padded = jnp.pad(solution, 1)
        along_x = cond_here * ((padded[cell_x + 1, cell_y, cell_z] - padded[cell_x - 1, cell_y, cell_z]) * 0.5)
        along_y = cond_here * ((padded[cell_x, cell_y + 1, cell_z] - padded[cell_x, cell_y - 1, cell_z]) * 0.5)
        along_z = cond_here * ((padded[cell_x, cell_y, cell_z + 1] - padded[cell_x, cell_y, cell_z - 1]) * 0.5)
        return jnp.stack([along_x, along_y, along_z])

    leadfield = jnp.transpose(lax.map(one_sensor, source_term), (1, 0, 2))
    projections = jnp.einsum("csp,st->ctp", leadfield, sensor_data, precision=lax.Precision.HIGHEST)
    return projections, gram_rows(leadfield)
```

```python
import functools

import jax
import jax.numpy as jnp
from jax import lax
from jax.experimental import pallas as pl
from jax.experimental.pallas import tpu as pltpu
from jax.sharding import PartitionSpec as P

F32 = jnp.float32
BF16 = jnp.bfloat16
MASS = 0.25
PAIRS = ((0, 0), (1, 1), (2, 2), (0, 1), (0, 2), (1, 2))
AXES = ("gx", "gy", "gz")


class Exchange:
    def __init__(self, send, recv):
        self.send, self.recv, self.used = send, recv, 0

    def start(self, source, target, axis, partner):
        copy = pltpu.make_async_remote_copy(
            src_ref=source,
            dst_ref=target,
            send_sem=self.send.at[self.used],
            recv_sem=self.recv.at[self.used],
            device_id={axis: partner},
            device_id_type=pl.DeviceIdType.MESH,
        )
        self.used += 1
        copy.start()
        return copy


def copies_needed(sizes):
    lines = sum(n - 1 for n in sizes)
    return 18 + lines + 2 * (sizes[0] - 1) + 2 * (sizes[1] - 1)


def kernel(sizes, src, lab, table, send_map, slots, data, proj, gram,
           field, image, xr_b, xr_v, ys_b, ys_v, yr_b, yr_v, zs_b, zs_v, zr_b, zr_v, zm,
           lys, lxr, lyr, lzr, wts, ghi, glo, onehot, pick, raw, turned,
           line_b, line_v, mid_b, mid_v, out_b, out_v, fin_b, fin_v, mq, red_x, red_y, red_z,
           load_sem, send_sem, recv_sem):
    nx, ny, nz = sizes
    count = dict(zip(AXES, sizes))
    me = {axis: lax.axis_index(axis) for axis in AXES}
    low = {axis: lax.rem(me[axis] + count[axis] - 1, count[axis]) for axis in AXES}
    high = {axis: lax.rem(me[axis] + 1, count[axis]) for axis in AXES}
    has_low = {axis: me[axis] > 0 for axis in AXES}
    has_high = {axis: me[axis] < count[axis] - 1 for axis in AXES}
    keep_low = {axis: jnp.where(has_low[axis], 1.0, 0.0).astype(F32) for axis in AXES}
    keep_high = {axis: jnp.where(has_high[axis], 1.0, 0.0).astype(F32) for axis in AXES}
    sensors, cells_xy, lanes = field.shape
    cx, cy = cells_xy // 8, 8
    cap = send_map.shape[1] // (nx * ny)
    total_slots = send_map.shape[1]
    ex = Exchange(send_sem, recv_sem)
    lane = lax.broadcasted_iota(jnp.int32, (8, lanes), 1)
    row = lax.broadcasted_iota(jnp.int32, (8, lanes), 0)

    load = pltpu.make_async_copy(src, field, load_sem)
    load.start()
    barrier = pltpu.get_barrier_semaphore()
    for axis in AXES:
        for d in range(1, count[axis]):
            partner = lax.rem(me[axis] + d, count[axis])
            pl.semaphore_signal(
                barrier, inc=1, device_id={axis: partner}, device_id_type=pl.DeviceIdType.MESH
            )
    lys[0:cx, :] = lab[pl.ds(0, cx, stride=cy), :]
    lys[cx : 2 * cx, :] = lab[pl.ds(cy - 1, cx, stride=cy), :]
    load.wait()

    def pack(whole, ys, zs):
        for s in range(sensors):
            for side, y in enumerate((0, cy - 1)):
                ys[side, cx * s : cx * s + cx, :] = whole[s, pl.ds(y, cx, stride=cy), :]

        def one(s, acc):
            here = lax.shift_right_logical(lane, 1) == s
            return tuple(
                jnp.where(here, pltpu.roll(whole[s, 8 * x : 8 * x + 8, :], 2 * s + 1, 1), acc[x])
                for x in range(cx)
            )

        acc = lax.fori_loop(0, sensors, one, (jnp.zeros((8, lanes), F32),) * cx, unroll=4)
        for x in range(cx):
            zs[8 * x : 8 * x + 8, :] = acc[x]

    def faces(whole, xr, ys, yr, zs, zr):
        last = cells_xy - 8
        return [
            ex.start(whole.at[:, 0:8, :], xr.at[1], "gx", low["gx"]),
            ex.start(whole.at[:, last : last + 8, :], xr.at[0], "gx", high["gx"]),
            ex.start(ys.at[0], yr.at[1], "gy", low["gy"]),
            ex.start(ys.at[1], yr.at[0], "gy", high["gy"]),
            ex.start(zs, zr.at[1], "gz", low["gz"]),
            ex.start(zs, zr.at[0], "gz", high["gz"]),
        ]

    pack(field, ys_b, zs_b)
    pl.semaphore_wait(barrier, sum(n - 1 for n in sizes))
    label_copies = [
        ex.start(lab.at[0:8, :], lxr.at[1], "gx", low["gx"]),
        ex.start(lab.at[cells_xy - 8 : cells_xy, :], lxr.at[0], "gx", high["gx"]),
        ex.start(lys, lyr.at[1], "gy", low["gy"]),
        ex.start(lys, lyr.at[0], "gy", high["gy"]),
        ex.start(lab, lzr.at[1], "gz", low["gz"]),
        ex.start(lab, lzr.at[0], "gz", high["gz"]),
    ]
    first_copies = faces(field, xr_b, ys_b, yr_b, zs_b, zr_b)

    wanted = send_map[...]
    key = lax.shift_right_arithmetic(wanted, 10) * lanes + (wanted & (lanes - 1))
    y_of = lax.shift_right_arithmetic(wanted, 7) & (cy - 1)
    for x in range(cx):
        places = lax.broadcasted_iota(jnp.int32, (lanes, total_slots), 0) + x * lanes
        onehot[x * lanes : (x + 1) * lanes, :] = jnp.where(places == key, 1.0, 0.0).astype(BF16)
    rows_in = lax.broadcasted_iota(jnp.int32, (total_slots, slots.shape[1]), 0)
    pick[...] = jnp.where(rows_in == slots[...], 1.0, 0.0).astype(BF16)

    for copy in label_copies:
        copy.wait()

    def tissue(shifted):
        level = jnp.zeros(shifted.shape, F32)
        for k in range(table.shape[0]):
            level = level + jnp.where(shifted == k + 1, table[k], 0.0)
        return level, jnp.where(shifted > 0, 1.0, 0.0).astype(F32)

    shifted = [lab[8 * x : 8 * x + 8, :] + 1 for x in range(cx)]
    for x in range(cx):
        here = shifted[x]
        if x > 0:
            x_low = shifted[x - 1]
        else:
            x_low = jnp.where(has_low["gx"], lxr[0] + 1, 0)
        if x < cx - 1:
            x_high = shifted[x + 1]
        else:
            x_high = jnp.where(has_high["gx"], lxr[1] + 1, 0)
        row_low = jnp.where(has_low["gy"], lyr[0, cx + x : cx + x + 1, :] + 1, 0)
        row_high = jnp.where(has_high["gy"], lyr[1, x : x + 1, :] + 1, 0)
        y_low = jnp.where(row == 0, row_low, pltpu.roll(here, 1, 0))
        y_high = jnp.where(row == cy - 1, row_high, pltpu.roll(here, cy - 1, 0))
        side_low = jnp.where(has_low["gz"], lzr[0, 8 * x : 8 * x + 8, :] + 1, 0)
        side_high = jnp.where(has_high["gz"], lzr[1, 8 * x : 8 * x + 8, :] + 1, 0)
        z_low = pltpu.roll(jnp.where(lane == lanes - 1, side_low, here), 1, 1)
        z_high = pltpu.roll(jnp.where(lane == 0, side_high, here), lanes - 1, 1)
        own_cond, own_in = tissue(here)
        diagonal = jnp.full((8, lanes), MASS, F32)
        for k, beside in enumerate((x_low, x_high, y_low, y_high, z_low, z_high)):
            its_cond, its_in = tissue(beside)
            weight = 0.5 * (own_cond + its_cond) * own_in * its_in
            wts[k, 8 * x : 8 * x + 8, :] = weight
            diagonal = diagonal + weight
        wts[6, 8 * x : 8 * x + 8, :] = diagonal
        wts[7, 8 * x : 8 * x + 8, :] = 0.5 * own_cond

    def sweep(whole, xr, yr, zr, result):
        for x in range(cx):
            span = slice(8 * x, 8 * x + 8)
            zm[span, :] = jnp.where(
                (lane & 1) == 0, zr[0, span, :] * keep_low["gz"], zr[1, span, :] * keep_high["gz"]
            )

        def pair(i, carry):
            slopes = [[[None, None] for _ in range(cx)] for _ in range(3)]
            for k in range(2):
                s = 2 * i + k
                own = [whole[s, 8 * x : 8 * x + 8, :] for x in range(cx)]
                outer = [xr[0, s] * keep_low["gx"]] + own + [xr[1, s] * keep_high["gx"]]
                sums = [None, None, None]
                for x in range(cx):
                    span = slice(8 * x, 8 * x + 8)
                    u = own[x]
                    low_row = yr[0, pl.ds(s * cx + x, 1), :] * keep_low["gy"]
                    high_row = yr[1, pl.ds(s * cx + x, 1), :] * keep_high["gy"]
                    y_low = jnp.where(row == 0, low_row, pltpu.roll(u, 1, 0))
                    y_high = jnp.where(row == cy - 1, high_row, pltpu.roll(u, cy - 1, 0))
                    beyond = pltpu.roll(zm[span, :], lanes - 1 - 2 * s, 1)
                    z_low = pltpu.roll(jnp.where(lane == lanes - 1, beyond, u), 1, 1)
                    z_high = pltpu.roll(jnp.where(lane == 0, beyond, u), lanes - 1, 1)
                    near = (outer[x], outer[x + 2], y_low, y_high, z_low, z_high)
                    q = wts[6, span, :] * u
                    for n in range(6):
                        q = q - wts[n, span, :] * near[n]
                    half = wts[7, span, :]
                    for c in range(3):
                        slopes[c][x][k] = half * (near[2 * c + 1] - near[2 * c])
                    if result is not None:
                        result[s, span, :] = q
                        terms = (u * u, u * q, q * q)
                    else:
                        terms = (u * q,)
                    for n, term in enumerate(terms):
                        sums[n] = term if sums[n] is None else sums[n] + term
                first = 0 if result is not None else 3
                for n in range(3 if result is not None else 1):
                    mq[first + n, pl.ds(pl.multiple_of(8 * s, 8), 8), :] = sums[n]
            at = pl.ds(pl.multiple_of(16 * i, 16), 16)
            for c in range(3):
                for x in range(cx):
                    slope = jnp.concatenate(slopes[c][x], axis=0)
                    coarse = slope.astype(BF16)
                    ghi[c, at, x * lanes : (x + 1) * lanes] = coarse
                    glo[c, at, x * lanes : (x + 1) * lanes] = (slope - coarse.astype(F32)).astype(BF16)
            return carry

        lax.fori_loop(0, sensors // 2, pair, 0)

    def gather(line):
        parts = []
        for c in range(3):
            product = jnp.dot(ghi[c], onehot[...], preferred_element_type=F32) + jnp.dot(
                glo[c], onehot[...], preferred_element_type=F32
            )
            for h in range(total_slots // lanes):
                raw[h] = product[:, h * lanes : (h + 1) * lanes]
            for g in range(sensors // 8):
                halves = []
                for h in range(total_slots // lanes):
                    acc = None
                    for y in range(cy):
                        strip = raw[h, pl.ds(8 * cy * g + y, 8, stride=cy), :]
                        term = jnp.where(y_of[:, h * lanes : (h + 1) * lanes] == y, strip, 0.0)
                        acc = term if acc is None else acc + term
                    halves.append(acc)
                parts.append(jnp.concatenate(halves, axis=1))
        parts.append(jnp.zeros((lanes - 3 * sensors, total_slots), F32))
        turned[...] = jnp.concatenate(parts, axis=0).T
        for j in range(ny * cap):
            line[j * nx : (j + 1) * nx, :] = turned[pl.ds(j, nx, stride=ny * cap), :]

    def spread(source, target, axis):
        rows = source.shape[0] // count[axis]
        mine = pl.ds(pl.multiple_of(me[axis] * rows, rows), rows)
        copies = []
        for d in range(1, count[axis]):
            partner = lax.rem(me[axis] + d, count[axis])
            theirs = pl.ds(pl.multiple_of(partner * rows, rows), rows)
            copies.append(ex.start(source.at[theirs, :], target.at[mine, :], axis, partner))
        target[mine, :] = source[mine, :]
        return copies

    def regroup(mid, out):
        rows = ny * cap
        for ix in range(nx):
            out[ix * rows : (ix + 1) * rows, :] = mid[pl.ds(ix, rows, stride=nx), :]

    def reduce_start(buffer, value, axis):
        buffer[0] = value
        copies = []
        for d in range(1, count[axis]):
            partner = lax.rem(me[axis] + d, count[axis])
            copies.append(ex.start(buffer.at[0], buffer.at[d], axis, partner))
        return copies

    def reduce_end(buffer, copies):
        for copy in copies:
            copy.wait()
        value = buffer[0]
        for d in range(1, len(copies) + 1):
            value = value + buffer[d]
        return value

    for copy in first_copies:
        copy.wait()
    sweep(field, xr_b, yr_b, zr_b, image)
    pack(image, ys_v, zs_v)
    second_copies = faces(image, xr_v, ys_v, yr_v, zs_v, zr_v)
    gather(line_b)
    line_b_copies = spread(line_b, mid_b, "gy")
    for copy in second_copies:
        copy.wait()
    sweep(image, xr_v, yr_v, zr_v, None)

    rows = []
    for m in range(4):
        for g in range(sensors // 8):
            acc = None
            for y in range(cy):
                strip = mq[m, pl.ds(8 * cy * g + y, 8, stride=cy), :]
                acc = strip if acc is None else acc + strip
            rows.append(acc)
    partial = lax.dot_general(
        jnp.ones((8, lanes), F32),
        jnp.concatenate(rows, axis=0),
        (((1,), (1,)), ((), ())),
        precision=lax.Precision.HIGHEST,
        preferred_element_type=F32,
    )[0:1, :]
    z_copies = reduce_start(red_z, partial, "gz")
    gather(line_v)
    line_v_copies = spread(line_v, mid_v, "gy")
    x_copies = reduce_start(red_x, reduce_end(red_z, z_copies), "gx")
    for copy in line_b_copies:
        copy.wait()
    regroup(mid_b, out_b)
    out_b_copies = spread(out_b, fin_b, "gx")
    y_copies = reduce_start(red_y, reduce_end(red_x, x_copies), "gy")
    for copy in line_v_copies:
        copy.wait()
    regroup(mid_v, out_v)
    out_v_copies = spread(out_v, fin_v, "gx")

    moments = jnp.broadcast_to(reduce_end(red_y, y_copies), (8, lanes))
    group = lane // sensors
    full = []
    for m in range(4):
        value = moments
        for g in range(lanes // sensors):
            shift = (sensors * (g - m)) % lanes
            turn = pltpu.roll(moments, shift, 1) if shift else moments
            value = jnp.where(group == g, turn, value)
        full.append(value)
    zero, one, two, three = full
    first_step = zero / one
    residue = first_step * first_step * two - zero
    growth = 1.0 + residue / zero
    curvature = growth * growth * one - 2.0 * growth * first_step * two + first_step * first_step * three
    second_step = residue / curvature
    source_coef = (first_step + second_step * growth)[0:1, :]
    image_coef = (second_step * first_step)[0:1, :]

    for copy in out_b_copies + out_v_copies:
        copy.wait()
    columns = (source_coef * fin_b[...] - image_coef * fin_v[...]).T
    coarse = columns.astype(BF16)
    fine = (columns - coarse.astype(F32)).astype(BF16)
    owned = jnp.dot(coarse, pick[...], preferred_element_type=F32) + jnp.dot(
        fine, pick[...], preferred_element_type=F32
    )
    per_time = data[...].T
    parts = [owned[sensors * c : sensors * (c + 1), :] for c in range(3)]
    for c in range(3):
        proj[c] = jnp.dot(
            per_time, parts[c], precision=lax.Precision.HIGHEST, preferred_element_type=F32
        )
    for k, (a, b) in enumerate(PAIRS):
        gram[k : k + 1, :] = jnp.sum(parts[a] * parts[b], axis=0, keepdims=True)


def per_device(sizes, source_term, labels, table, send_map, owner_slots, sensor_data):
    sensors, cx, cy, lanes = source_term.shape
    cells_xy = cx * cy
    total = send_map.shape[-1]
    owned = owner_slots.shape[0]
    times = sensor_data.shape[1]
    n = copies_needed(sizes)
    vmem = pltpu.VMEM
    scratch = [
        vmem((sensors, cells_xy, lanes), F32),
        vmem((sensors, cells_xy, lanes), F32),
        vmem((2, sensors, 8, lanes), F32),
        vmem((2, sensors, 8, lanes), F32),
        vmem((2, sensors * cx, lanes), F32),
        vmem((2, sensors * cx, lanes), F32),
        vmem((2, sensors * cx, lanes), F32),
        vmem((2, sensors * cx, lanes), F32),
        vmem((cells_xy, lanes), F32),
        vmem((cells_xy, lanes), F32),
        vmem((2, cells_xy, lanes), F32),
        vmem((2, cells_xy, lanes), F32),
        vmem((cells_xy, lanes), F32),
        vmem((2 * cx, lanes), jnp.int32),
        vmem((2, 8, lanes), jnp.int32),
        vmem((2, 2 * cx, lanes), jnp.int32),
        vmem((2, cells_xy, lanes), jnp.int32),
        vmem((8, cells_xy, lanes), F32),
        vmem((3, sensors * 8, cx * lanes), BF16),
        vmem((3, sensors * 8, cx * lanes), BF16),
        vmem((cx * lanes, total), BF16),
        vmem((total, owned), BF16),
        vmem((total // lanes, sensors * 8, lanes), F32),
        vmem((total, lanes), F32),
    ]
    scratch += [vmem((total, lanes), F32)] * 8
    scratch += [
        vmem((4, sensors * 8, lanes), F32),
        vmem((sizes[0], 1, lanes), F32),
        vmem((sizes[1], 1, lanes), F32),
        vmem((sizes[2], 1, lanes), F32),
        pltpu.SemaphoreType.DMA,
        pltpu.SemaphoreType.DMA((n,)),
        pltpu.SemaphoreType.DMA((n,)),
    ]
    whole = pl.BlockSpec(memory_space=pltpu.VMEM)
    return pl.pallas_call(
        functools.partial(kernel, sizes),
        out_shape=(
            jax.ShapeDtypeStruct((3, times, owned), F32),
            jax.ShapeDtypeStruct((len(PAIRS), owned), F32),
        ),
        in_specs=[
            pl.BlockSpec(memory_space=pl.ANY),
            whole,
            pl.BlockSpec(memory_space=pltpu.SMEM),
            whole,
            whole,
            whole,
        ],
        out_specs=(whole, whole),
        scratch_shapes=scratch,
        compiler_params=pltpu.CompilerParams(
            collective_id=0, has_side_effects=True, vmem_limit_bytes=40 * 1024 * 1024
        ),
        name="solve",
    )(
        source_term.reshape(sensors, cells_xy, lanes),
        labels.reshape(cells_xy, lanes),
        table,
        send_map.reshape(1, total),
        owner_slots.reshape(1, owned),
        sensor_data,
    )


def solution(mesh):
    sizes = tuple(mesh.shape[axis] for axis in AXES)
    in_specs = (
        P(None, "gx", "gy", "gz"),
        P("gx", "gy", "gz"),
        P(),
        P("gx", "gy", "gz", None),
        P(AXES),
        P(),
    )
    out_specs = (P(None, None, AXES), P(None, AXES))
    return jax.shard_map(
        functools.partial(per_device, sizes),
        mesh=mesh,
        in_specs=in_specs,
        out_specs=out_specs,
        check_vma=False,
    )
```

```python
import functools

import jax
import jax.numpy as jnp
from jax import lax
from jax.experimental import pallas as pl
from jax.experimental.pallas import tpu as pltpu
from jax.sharding import PartitionSpec as P

F32 = jnp.float32
BF16 = jnp.bfloat16
MASS = 0.25
PAIRS = ((0, 0), (1, 1), (2, 2), (0, 1), (0, 2), (1, 2))
AXES = ("gx", "gy", "gz")


class Exchange:
    def __init__(self, send, recv):
        self.send, self.recv, self.used = send, recv, 0

    def start(self, source, target, axis, partner):
        return self.start_at(source, target, {axis: partner})

    def start_at(self, source, target, where):
        copy = pltpu.make_async_remote_copy(
            src_ref=source,
            dst_ref=target,
            send_sem=self.send.at[self.used],
            recv_sem=self.recv.at[self.used],
            device_id=where,
            device_id_type=pl.DeviceIdType.MESH,
        )
        self.used += 1
        copy.start()
        return copy


CHUNKS = 2


def copies_needed(sizes):
    nx, ny, nz = sizes
    plane = nx * nz - 1
    return 6 + 2 * (4 * CHUNKS + 2) + plane + 3 * (ny - 1) + 2 * (nx - 1)


def waves_needed(sizes):
    nx, ny, nz = sizes
    return max(nx // 2 - 1 + nz // 2, ny // 2 - 1)


def kernel(sizes, src, lab_in, table_in, send_in, slots_in, moments_out, owned_b_out, owned_v_out,
           lab, table, send_map, slots, field, image, xr_b, xr_v, ys_b, ys_v, yr_b, yr_v,
           zs_b, zs_v, zr_b, zr_v, zm, lys, lxr, lyr, lzr, wts, ghi, glo, onehot, pick, raw, turned,
           line_b, line_v, mid_b, mid_v, out_b, out_v, fin_b, fin_v, mq, red_plane, red_line,
           load_sem, send_sem, recv_sem, wave_sem):
    nx, ny, nz = sizes
    count = dict(zip(AXES, sizes))
    me = {axis: lax.axis_index(axis) for axis in AXES}
    low = {axis: lax.rem(me[axis] + count[axis] - 1, count[axis]) for axis in AXES}
    high = {axis: lax.rem(me[axis] + 1, count[axis]) for axis in AXES}
    has_low = {axis: me[axis] > 0 for axis in AXES}
    has_high = {axis: me[axis] < count[axis] - 1 for axis in AXES}
    keep_low = {axis: jnp.where(has_low[axis], 1.0, 0.0).astype(F32) for axis in AXES}
    keep_high = {axis: jnp.where(has_high[axis], 1.0, 0.0).astype(F32) for axis in AXES}
    sensors, cells_xy, lanes = field.shape
    cx, cy = cells_xy // 8, 8
    total_slots = send_map.shape[1]
    cap = total_slots // (nx * ny)
    per_chunk = sensors // CHUNKS
    ex = Exchange(send_sem, recv_sem)
    lane = lax.broadcasted_iota(jnp.int32, (8, lanes), 1)
    row = lax.broadcasted_iota(jnp.int32, (8, lanes), 0)

    def tell(sem, axis, partner):
        pl.semaphore_signal(
            sem, inc=1, device_id={axis: partner}, device_id_type=pl.DeviceIdType.MESH
        )

    barrier = pltpu.get_barrier_semaphore()
    for axis in AXES:
        tell(barrier, axis, low[axis])
        tell(barrier, axis, high[axis])
    loads = [pltpu.make_async_copy(lab_in, lab, load_sem.at[0])]
    for h in range(CHUNKS):
        part = pl.ds(per_chunk * h, per_chunk)
        loads.append(pltpu.make_async_copy(src.at[part], field.at[part], load_sem.at[1 + h]))
    for k, (a, b) in enumerate(((table_in, table), (send_in, send_map), (slots_in, slots))):
        loads.append(pltpu.make_async_copy(a, b, load_sem.at[1 + CHUNKS + k]))
    for copy in loads:
        copy.start()

    steps = {"gx": nx // 2 - 1, "gz": nz // 2, "gy": ny // 2 - 1}
    plan = [[] for _ in range(waves_needed(sizes))]
    for k in range(steps["gx"]):
        plan[k].append("gx")
    for k in range(steps["gz"]):
        plan[steps["gx"] + k].append("gz")
    for k in range(steps["gy"]):
        plan[k].append("gy")
    wave_at = [0]

    def wave_send():
        if wave_at[0] < len(plan):
            for axis in plan[wave_at[0]]:
                k = AXES.index(axis)
                tell(wave_sem.at[2 * k], axis, low[axis])
                tell(wave_sem.at[2 * k + 1], axis, high[axis])

    def wave(times=1):
        for _ in range(times):
            if wave_at[0] < len(plan):
                for axis in plan[wave_at[0]]:
                    k = AXES.index(axis)
                    pl.semaphore_wait(wave_sem.at[2 * k], 1)
                    pl.semaphore_wait(wave_sem.at[2 * k + 1], 1)
                wave_at[0] += 1
                wave_send()

    def x_faces(whole, xr, h):
        part = pl.ds(per_chunk * h, per_chunk)
        last = cells_xy - 8
        return [
            ex.start(whole.at[part, 0:8, :], xr.at[1, part], "gx", low["gx"]),
            ex.start(whole.at[part, last : last + 8, :], xr.at[0, part], "gx", high["gx"]),
        ]

    def y_faces(ys, yr, h):
        part = pl.ds(per_chunk * h * cx, per_chunk * cx)
        return [
            ex.start(ys.at[0, part], yr.at[1, part], "gy", low["gy"]),
            ex.start(ys.at[1, part], yr.at[0, part], "gy", high["gy"]),
        ]

    def z_faces(zs, zr):
        return [
            ex.start(zs, zr.at[1], "gz", low["gz"]),
            ex.start(zs, zr.at[0], "gz", high["gz"]),
        ]

    def pack_z(values, s, acc):
        here = lax.shift_right_logical(lane, 1) == s
        return tuple(
            jnp.where(here, pltpu.roll(values[x], 2 * s + 1, 1), acc[x]) for x in range(cx)
        )

    def store_z(zs, acc):
        for x in range(cx):
            zs[8 * x : 8 * x + 8, :] = acc[x]

    no_z = (jnp.zeros((8, lanes), F32),) * cx

    loads[0].wait()
    lys[0:cx, :] = lab[pl.ds(0, cx, stride=cy), :]
    lys[cx : 2 * cx, :] = lab[pl.ds(cy - 1, cx, stride=cy), :]
    for copy in loads[1:]:
        copy.wait()
    pl.semaphore_wait(barrier, 2 * len(AXES))
    wave_send()
    first_x = [x_faces(field, xr_b, h) for h in range(CHUNKS)]
    label_copies = [
        ex.start(lab.at[0:8, :], lxr.at[1], "gx", low["gx"]),
        ex.start(lab.at[cells_xy - 8 : cells_xy, :], lxr.at[0], "gx", high["gx"]),
        ex.start(lys, lyr.at[1], "gy", low["gy"]),
        ex.start(lys, lyr.at[0], "gy", high["gy"]),
        ex.start(lab, lzr.at[1], "gz", low["gz"]),
        ex.start(lab, lzr.at[0], "gz", high["gz"]),
    ]
    first_y = []
    for h in range(CHUNKS):
        for s in range(per_chunk * h, per_chunk * (h + 1)):
            for side, y in enumerate((0, cy - 1)):
                ys_b[side, cx * s : cx * s + cx, :] = field[s, pl.ds(y, cx, stride=cy), :]
        first_y.append(y_faces(ys_b, yr_b, h))
    store_z(
        zs_b,
        lax.fori_loop(
            0,
            sensors,
            lambda s, acc: pack_z([field[s, 8 * x : 8 * x + 8, :] for x in range(cx)], s, acc),
            no_z,
            unroll=4,
        ),
    )
    first_z = z_faces(zs_b, zr_b)

    wanted = send_map[...]
    key = lax.shift_right_arithmetic(wanted, 10) * lanes + (wanted & (lanes - 1))
    y_of = lax.shift_right_arithmetic(wanted, 7) & (cy - 1)
    for x in range(cx):
        places = lax.broadcasted_iota(jnp.int32, (lanes, total_slots), 0) + x * lanes
        onehot[x * lanes : (x + 1) * lanes, :] = jnp.where(places == key, 1.0, 0.0).astype(BF16)
    rows_in = lax.broadcasted_iota(jnp.int32, (total_slots, slots.shape[1]), 0)
    pick[...] = jnp.where(rows_in == slots[...], 1.0, 0.0).astype(BF16)
    wave(2)

    for copy in label_copies:
        copy.wait()

    def tissue(shifted):
        level = jnp.zeros(shifted.shape, F32)
        for k in range(table.shape[0]):
            level = level + jnp.where(shifted == k + 1, table[k], 0.0)
        return level, jnp.where(shifted > 0, 1.0, 0.0).astype(F32)

    shifted = [lab[8 * x : 8 * x + 8, :] + 1 for x in range(cx)]
    for x in range(cx):
        here = shifted[x]
        if x > 0:
            x_low = shifted[x - 1]
        else:
            x_low = jnp.where(has_low["gx"], lxr[0] + 1, 0)
        if x < cx - 1:
            x_high = shifted[x + 1]
        else:
            x_high = jnp.where(has_high["gx"], lxr[1] + 1, 0)
        row_low = jnp.where(has_low["gy"], lyr[0, cx + x : cx + x + 1, :] + 1, 0)
        row_high = jnp.where(has_high["gy"], lyr[1, x : x + 1, :] + 1, 0)
        y_low = jnp.where(row == 0, row_low, pltpu.roll(here, 1, 0))
        y_high = jnp.where(row == cy - 1, row_high, pltpu.roll(here, cy - 1, 0))
        side_low = jnp.where(has_low["gz"], lzr[0, 8 * x : 8 * x + 8, :] + 1, 0)
        side_high = jnp.where(has_high["gz"], lzr[1, 8 * x : 8 * x + 8, :] + 1, 0)
        z_low = pltpu.roll(jnp.where(lane == lanes - 1, side_low, here), 1, 1)
        z_high = pltpu.roll(jnp.where(lane == 0, side_high, here), lanes - 1, 1)
        own_cond, own_in = tissue(here)
        diagonal = jnp.full((8, lanes), MASS, F32)
        for k, beside in enumerate((x_low, x_high, y_low, y_high, z_low, z_high)):
            its_cond, its_in = tissue(beside)
            weight = 0.5 * (own_cond + its_cond) * own_in * its_in
            wts[k, 8 * x : 8 * x + 8, :] = weight
            diagonal = diagonal + weight
        wts[6, 8 * x : 8 * x + 8, :] = diagonal
        wts[7, 8 * x : 8 * x + 8, :] = 0.5 * own_cond
    wave()

    def merge_z(zr):
        for x in range(cx):
            span = slice(8 * x, 8 * x + 8)
            zm[span, :] = jnp.where(
                (lane & 1) == 0, zr[0, span, :] * keep_low["gz"], zr[1, span, :] * keep_high["gz"]
            )

    def neighbours(whole, xr, yr, s):
        own = [whole[s, 8 * x : 8 * x + 8, :] for x in range(cx)]
        outer = [xr[0, s] * keep_low["gx"]] + own + [xr[1, s] * keep_high["gx"]]
        near = []
        for x in range(cx):
            u = own[x]
            low_row = yr[0, pl.ds(s * cx + x, 1), :] * keep_low["gy"]
            high_row = yr[1, pl.ds(s * cx + x, 1), :] * keep_high["gy"]
            y_low = jnp.where(row == 0, low_row, pltpu.roll(u, 1, 0))
            y_high = jnp.where(row == cy - 1, high_row, pltpu.roll(u, cy - 1, 0))
            beyond = pltpu.roll(zm[8 * x : 8 * x + 8, :], lanes - 1 - 2 * s, 1)
            z_low = pltpu.roll(jnp.where(lane == lanes - 1, beyond, u), 1, 1)
            z_high = pltpu.roll(jnp.where(lane == 0, beyond, u), lanes - 1, 1)
            near.append((outer[x], outer[x + 2], y_low, y_high, z_low, z_high))
        return own, near

    def apply(own, near, x):
        span = slice(8 * x, 8 * x + 8)
        q = wts[6, span, :] * own[x]
        for n in range(6):
            q = q - wts[n, span, :] * near[x][n]
        return q

    def rows_of(s):
        return pl.ds(pl.multiple_of(8 * s, 8), 8)

    def image_pass(i, acc):
        for k in range(2):
            s = 2 * i + k
            own, near = neighbours(field, xr_b, yr_b, s)
            results = [apply(own, near, x) for x in range(cx)]
            for x in range(cx):
                image[s, 8 * x : 8 * x + 8, :] = results[x]
                ys_v[0, pl.ds(s * cx + x, 1), :] = results[x][0:1, :]
                ys_v[1, pl.ds(s * cx + x, 1), :] = results[x][cy - 1 : cy, :]
            acc = pack_z(results, s, acc)
        return acc

    def energy_pass(i, carry):
        for k in range(2):
            s = 2 * i + k
            own, near = neighbours(image, xr_v, yr_v, s)
            term = own[0] * apply(own, near, 0)
            for x in range(1, cx):
                term = term + own[x] * apply(own, near, x)
            mq[3, rows_of(s), :] = term
        return carry

    def slope_pass(whole, xr, yr, result, i):
        slopes = [[[None, None] for _ in range(cx)] for _ in range(3)]
        for k in range(2):
            s = 2 * i + k
            own, near = neighbours(whole, xr, yr, s)
            sums = [None, None, None]
            for x in range(cx):
                half = wts[7, 8 * x : 8 * x + 8, :]
                for c in range(3):
                    slopes[c][x][k] = half * (near[x][2 * c + 1] - near[x][2 * c])
                if result is not None:
                    q = result[s, 8 * x : 8 * x + 8, :]
                    for n, term in enumerate((own[x] * own[x], own[x] * q, q * q)):
                        sums[n] = term if sums[n] is None else sums[n] + term
            if result is not None:
                for n in range(3):
                    mq[n, rows_of(s), :] = sums[n]
        at = pl.ds(pl.multiple_of(16 * i, 16), 16)
        for c in range(3):
            for x in range(cx):
                slope = jnp.concatenate(slopes[c][x], axis=0)
                coarse = slope.astype(BF16)
                ghi[c, at, x * lanes : (x + 1) * lanes] = coarse
                glo[c, at, x * lanes : (x + 1) * lanes] = (slope - coarse.astype(F32)).astype(BF16)

    def slopes_of(whole, xr, yr, result):
        def step(i, carry):
            slope_pass(whole, xr, yr, result, i)
            return carry

        lax.fori_loop(0, sensors // 2, step, 0)

    def gather(line):
        parts = []
        for c in range(3):
            product = jnp.dot(ghi[c], onehot[...], preferred_element_type=F32) + jnp.dot(
                glo[c], onehot[...], preferred_element_type=F32
            )
            for h in range(total_slots // lanes):
                raw[h] = product[:, h * lanes : (h + 1) * lanes]
            for g in range(sensors // 8):
                halves = []
                for h in range(total_slots // lanes):
                    acc = None
                    for y in range(cy):
                        strip = raw[h, pl.ds(8 * cy * g + y, 8, stride=cy), :]
                        term = jnp.where(y_of[:, h * lanes : (h + 1) * lanes] == y, strip, 0.0)
                        acc = term if acc is None else acc + term
                    halves.append(acc)
                parts.append(jnp.concatenate(halves, axis=1))
        parts.append(jnp.zeros((lanes - 3 * sensors, total_slots), F32))
        turned[...] = jnp.concatenate(parts, axis=0).T
        for j in range(ny * cap):
            line[j * nx : (j + 1) * nx, :] = turned[pl.ds(j, nx, stride=ny * cap), :]

    def spread(source, target, axis):
        rows = source.shape[0] // count[axis]
        mine = pl.ds(pl.multiple_of(me[axis] * rows, rows), rows)
        copies = []
        for d in range(1, count[axis]):
            partner = lax.rem(me[axis] + d, count[axis])
            theirs = pl.ds(pl.multiple_of(partner * rows, rows), rows)
            copies.append(ex.start(source.at[theirs, :], target.at[mine, :], axis, partner))
        target[mine, :] = source[mine, :]
        return copies

    def regroup(mid, out):
        rows = ny * cap
        for ix in range(nx):
            out[ix * rows : (ix + 1) * rows, :] = mid[pl.ds(ix, rows, stride=nx), :]

    def reduce_start(buffer, value, partners):
        buffer[0] = value
        return [
            ex.start_at(buffer.at[0], buffer.at[k + 1], where) for k, where in enumerate(partners)
        ]

    def reduce_end(buffer, copies):
        for copy in copies:
            copy.wait()
        value = buffer[0]
        for d in range(1, len(copies) + 1):
            value = value + buffer[d]
        return value

    def moment_rows(m):
        parts = []
        for g in range(sensors // 8):
            acc = None
            for y in range(cy):
                strip = mq[m, pl.ds(8 * cy * g + y, 8, stride=cy), :]
                acc = strip if acc is None else acc + strip
            parts.append(acc)
        return parts

    def lane_sums(parts):
        return lax.dot_general(
            jnp.ones((8, lanes), F32),
            jnp.concatenate(parts, axis=0),
            (((1,), (1,)), ((), ())),
            precision=lax.Precision.HIGHEST,
            preferred_element_type=F32,
        )[0:1, :]

    def select(fin):
        columns = fin[...].T
        coarse = columns.astype(BF16)
        fine = (columns - coarse.astype(F32)).astype(BF16)
        return jnp.dot(coarse, pick[...], preferred_element_type=F32) + jnp.dot(
            fine, pick[...], preferred_element_type=F32
        )

    def wait(copies):
        for copy in copies:
            copy.wait()

    blank = [jnp.zeros((8, lanes), F32)]
    half_pairs = per_chunk // 2
    wait(first_z)
    merge_z(zr_b)
    acc = no_z
    second = []
    for h in range(CHUNKS):
        wait(first_x[h] + first_y[h])
        acc = lax.fori_loop(half_pairs * h, half_pairs * (h + 1), image_pass, acc)
        second.append(x_faces(image, xr_v, h) + y_faces(ys_v, yr_v, h))
    store_z(zs_v, acc)
    second_z = z_faces(zs_v, zr_v)
    wave()
    slopes_of(field, xr_b, yr_b, image)
    wave()
    early = lane_sums(moment_rows(0) + moment_rows(1) + moment_rows(2) + blank * (sensors // 8))
    gather(line_b)
    wave(len(plan))
    line_b_copies = spread(line_b, mid_b, "gy")
    wait(second_z)
    merge_z(zr_v)
    for h in range(CHUNKS):
        wait(second[h])
        lax.fori_loop(half_pairs * h, half_pairs * (h + 1), energy_pass, 0)
    partial = early + lane_sums(blank * (3 * sensors // 8) + moment_rows(3))
    plane = [
        {"gx": lax.rem(me["gx"] + dx, nx), "gz": lax.rem(me["gz"] + dz, nz)}
        for dx in range(nx)
        for dz in range(nz)
        if dx or dz
    ]
    plane_copies = reduce_start(red_plane, partial, plane)
    slopes_of(image, xr_v, yr_v, None)
    gather(line_v)
    line_v_copies = spread(line_v, mid_v, "gy")
    line = [{"gy": lax.rem(me["gy"] + d, ny)} for d in range(1, ny)]
    line_copies = reduce_start(red_line, reduce_end(red_plane, plane_copies), line)
    wait(line_b_copies)
    regroup(mid_b, out_b)
    out_b_copies = spread(out_b, fin_b, "gx")
    wait(line_v_copies)
    regroup(mid_v, out_v)
    out_v_copies = spread(out_v, fin_v, "gx")
    wait(out_b_copies)
    owned_b_out[...] = select(fin_b)
    wait(out_v_copies)
    owned_v_out[...] = select(fin_v)
    moments_out[...] = jnp.broadcast_to(reduce_end(red_line, line_copies), (8, lanes))


def finish(moments_in, owned_b, owned_v, data, proj, gram):
    sensors = data.shape[0]
    moments = moments_in[...]
    lanes = moments.shape[1]
    group = lax.broadcasted_iota(jnp.int32, moments.shape, 1) // sensors
    full = []
    for m in range(4):
        value = moments
        for g in range(lanes // sensors):
            shift = (sensors * (g - m)) % lanes
            turn = pltpu.roll(moments, shift, 1) if shift else moments
            value = jnp.where(group == g, turn, value)
        full.append(value)
    zero, one, two, three = full
    first_step = zero / one
    residue = first_step * first_step * two - zero
    growth = 1.0 + residue / zero
    curvature = growth * growth * one - 2.0 * growth * first_step * two + first_step * first_step * three
    second_step = residue / curvature
    source_coef = (first_step + second_step * growth)[0:1, :]
    image_coef = (second_step * first_step)[0:1, :]
    down = (lanes, lanes)
    owned = jnp.broadcast_to(source_coef, down).T * owned_b[...] - jnp.broadcast_to(image_coef, down).T * owned_v[...]
    per_time = data[...].T
    parts = [owned[sensors * c : sensors * (c + 1), :] for c in range(3)]
    for c in range(3):
        proj[c] = jnp.dot(
            per_time, parts[c], precision=lax.Precision.HIGHEST, preferred_element_type=F32
        )
    for k, (a, b) in enumerate(PAIRS):
        gram[k : k + 1, :] = jnp.sum(parts[a] * parts[b], axis=0, keepdims=True)


def per_device(sizes, source_term, labels, table, send_map, owner_slots, sensor_data):
    sensors, cx, cy, lanes = source_term.shape
    cells_xy = cx * cy
    total = send_map.shape[-1]
    owned = owner_slots.shape[0]
    times = sensor_data.shape[1]
    n = copies_needed(sizes)
    vmem = pltpu.VMEM
    scratch = [
        vmem((cells_xy, lanes), jnp.int32),
        pltpu.SMEM(table.shape, F32),
        vmem((1, total), jnp.int32),
        vmem((1, owned), jnp.int32),
        vmem((sensors, cells_xy, lanes), F32),
        vmem((sensors, cells_xy, lanes), F32),
        vmem((2, sensors, 8, lanes), F32),
        vmem((2, sensors, 8, lanes), F32),
        vmem((2, sensors * cx, lanes), F32),
        vmem((2, sensors * cx, lanes), F32),
        vmem((2, sensors * cx, lanes), F32),
        vmem((2, sensors * cx, lanes), F32),
        vmem((cells_xy, lanes), F32),
        vmem((cells_xy, lanes), F32),
        vmem((2, cells_xy, lanes), F32),
        vmem((2, cells_xy, lanes), F32),
        vmem((cells_xy, lanes), F32),
        vmem((2 * cx, lanes), jnp.int32),
        vmem((2, 8, lanes), jnp.int32),
        vmem((2, 2 * cx, lanes), jnp.int32),
        vmem((2, cells_xy, lanes), jnp.int32),
        vmem((8, cells_xy, lanes), F32),
        vmem((3, sensors * 8, cx * lanes), BF16),
        vmem((3, sensors * 8, cx * lanes), BF16),
        vmem((cx * lanes, total), BF16),
        vmem((total, owned), BF16),
        vmem((total // lanes, sensors * 8, lanes), F32),
        vmem((total, lanes), F32),
    ]
    scratch += [vmem((total, lanes), F32)] * 8
    scratch += [
        vmem((4, sensors * 8, lanes), F32),
        vmem((sizes[0] * sizes[2], 1, lanes), F32),
        vmem((sizes[1], 1, lanes), F32),
        pltpu.SemaphoreType.DMA((4 + CHUNKS,)),
        pltpu.SemaphoreType.DMA((n,)),
        pltpu.SemaphoreType.DMA((n,)),
        pltpu.SemaphoreType.REGULAR((2 * len(AXES),)),
    ]
    whole = pl.BlockSpec(memory_space=pltpu.VMEM)
    moments, owned_b, owned_v = pl.pallas_call(
        functools.partial(kernel, sizes),
        out_shape=(
            jax.ShapeDtypeStruct((8, lanes), F32),
            jax.ShapeDtypeStruct((lanes, owned), F32),
            jax.ShapeDtypeStruct((lanes, owned), F32),
        ),
        in_specs=[pl.BlockSpec(memory_space=pltpu.HBM)] * 5,
        out_specs=(whole,) * 3,
        scratch_shapes=scratch,
        compiler_params=pltpu.CompilerParams(
            collective_id=0, has_side_effects=True, vmem_limit_bytes=40 * 1024 * 1024
        ),
        name="solve",
    )(
        *(
            pltpu.with_memory_space_constraint(operand, pltpu.HBM)
            for operand in (
                source_term.reshape(sensors, cells_xy, lanes),
                labels.reshape(cells_xy, lanes),
                table,
                send_map.reshape(1, total),
                owner_slots.reshape(1, owned),
            )
        )
    )
    return pl.pallas_call(
        finish,
        out_shape=(
            jax.ShapeDtypeStruct((3, times, owned), F32),
            jax.ShapeDtypeStruct((len(PAIRS), owned), F32),
        ),
        in_specs=[whole] * 4,
        out_specs=(whole, whole),
        compiler_params=pltpu.CompilerParams(vmem_limit_bytes=40 * 1024 * 1024),
        name="finish",
    )(moments, owned_b, owned_v, sensor_data)


def solution(mesh):
    sizes = tuple(mesh.shape[axis] for axis in AXES)
    in_specs = (
        P(None, "gx", "gy", "gz"),
        P("gx", "gy", "gz"),
        P(),
        P("gx", "gy", "gz", None),
        P(AXES),
        P(),
    )
    out_specs = (P(None, None, AXES), P(None, AXES))
    return jax.shard_map(
        functools.partial(per_device, sizes),
        mesh=mesh,
        in_specs=in_specs,
        out_specs=out_specs,
        check_vma=False,
    )
```

```python
import functools

import jax
import jax.numpy as jnp
from jax import lax
from jax.experimental import pallas as pl
from jax.experimental.pallas import tpu as pltpu
from jax.sharding import PartitionSpec as P

F32 = jnp.float32
BF16 = jnp.bfloat16
MASS = 0.25
PAIRS = ((0, 0), (1, 1), (2, 2), (0, 1), (0, 2), (1, 2))
AXES = ("gx", "gy", "gz")


class Exchange:
    def __init__(self, send, recv):
        self.send, self.recv, self.used = send, recv, 0

    def start(self, source, target, axis, partner):
        return self.start_at(source, target, {axis: partner})

    def start_at(self, source, target, where):
        copy = pltpu.make_async_remote_copy(
            src_ref=source,
            dst_ref=target,
            send_sem=self.send.at[self.used],
            recv_sem=self.recv.at[self.used],
            device_id=where,
            device_id_type=pl.DeviceIdType.MESH,
        )
        self.used += 1
        copy.start()
        return copy


CHUNKS = 2
UNROLL = 8


def copies_needed(sizes):
    nx, ny, nz = sizes
    plane = nx * nz - 1
    return 6 + 2 * (4 * CHUNKS + 2) + plane + 3 * (ny - 1) + 2 * (nx - 1)


def doubling(known, size):
    strides = []
    while known < size // 2:
        strides.append(max(known, 1))
        known += strides[-1]
    return strides


def wave_plan(sizes):
    nx, ny, nz = sizes
    across = [("gx", d) for d in doubling(1, nx)] + [("gz", d) for d in doubling(0, nz)]
    along = [("gy", d) for d in doubling(1, ny)]
    plan = [[] for _ in range(max(len(across), len(along)))]
    for steps in (across, along):
        for k, step in enumerate(steps):
            plan[k].append(step)
    return plan


def kernel(sizes, src, lab_in, table_in, send_in, slots_in, moments_out, owned_b_out, owned_v_out,
           lab, table, send_map, slots, field, image, xr_b, xr_v, ys_b, ys_v, yr_b, yr_v,
           zs_b, zs_v, zr_b, zr_v, zm, lys, lxr, lyr, lzr, wts, ghi, glo, onehot, pick, raw,
           line_b, line_v, mid_b, mid_v, out_b, out_v, fin_b, fin_v, mq, red_plane, red_line,
           load_sem, send_sem, recv_sem, wave_sem):
    nx, ny, nz = sizes
    count = dict(zip(AXES, sizes))
    me = {axis: lax.axis_index(axis) for axis in AXES}
    low = {axis: lax.rem(me[axis] + count[axis] - 1, count[axis]) for axis in AXES}
    high = {axis: lax.rem(me[axis] + 1, count[axis]) for axis in AXES}
    has_low = {axis: me[axis] > 0 for axis in AXES}
    has_high = {axis: me[axis] < count[axis] - 1 for axis in AXES}
    keep_low = {axis: jnp.where(has_low[axis], 1.0, 0.0).astype(F32) for axis in AXES}
    keep_high = {axis: jnp.where(has_high[axis], 1.0, 0.0).astype(F32) for axis in AXES}
    sensors, cells_xy, lanes = field.shape
    cx, cy = cells_xy // 8, 8
    total_slots = send_map.shape[1]
    cap = total_slots // (nx * ny)
    per_chunk = sensors // CHUNKS
    ex = Exchange(send_sem, recv_sem)
    lane = lax.broadcasted_iota(jnp.int32, (8, lanes), 1)
    row = lax.broadcasted_iota(jnp.int32, (8, lanes), 0)

    def tell(sem, axis, partner):
        pl.semaphore_signal(
            sem, inc=1, device_id={axis: partner}, device_id_type=pl.DeviceIdType.MESH
        )

    barrier = pltpu.get_barrier_semaphore()
    for axis in AXES:
        tell(barrier, axis, low[axis])
        tell(barrier, axis, high[axis])
    loads = [pltpu.make_async_copy(lab_in, lab, load_sem.at[0])]
    for h in range(CHUNKS):
        part = pl.ds(per_chunk * h, per_chunk)
        loads.append(pltpu.make_async_copy(src.at[part], field.at[part], load_sem.at[1 + h]))
    for k, (a, b) in enumerate(((table_in, table), (send_in, send_map), (slots_in, slots))):
        loads.append(pltpu.make_async_copy(a, b, load_sem.at[1 + CHUNKS + k]))
    for copy in loads:
        copy.start()

    plan = wave_plan(sizes)
    wave_at = [0]

    def wave_sems(k, axis):
        first = 2 * (len(AXES) * k + AXES.index(axis))
        return wave_sem.at[first], wave_sem.at[first + 1]

    def wave_send():
        k = wave_at[0]
        if k < len(plan):
            for axis, stride in plan[k]:
                down, up = wave_sems(k, axis)
                tell(down, axis, lax.rem(me[axis] + count[axis] - stride, count[axis]))
                tell(up, axis, lax.rem(me[axis] + stride, count[axis]))

    def wave(times=1):
        for _ in range(times):
            k = wave_at[0]
            if k < len(plan):
                for axis, _stride in plan[k]:
                    for sem in wave_sems(k, axis):
                        pl.semaphore_wait(sem, 1)
                wave_at[0] += 1
                wave_send()

    def x_faces(whole, xr, h):
        part = pl.ds(per_chunk * h, per_chunk)
        last = cells_xy - 8
        return [
            ex.start(whole.at[part, 0:8, :], xr.at[1, part], "gx", low["gx"]),
            ex.start(whole.at[part, last : last + 8, :], xr.at[0, part], "gx", high["gx"]),
        ]

    def y_faces(ys, yr, h):
        part = pl.ds(per_chunk * h * cx, per_chunk * cx)
        return [
            ex.start(ys.at[0, part], yr.at[1, part], "gy", low["gy"]),
            ex.start(ys.at[1, part], yr.at[0, part], "gy", high["gy"]),
        ]

    def z_faces(zs, zr):
        return [
            ex.start(zs, zr.at[1], "gz", low["gz"]),
            ex.start(zs, zr.at[0], "gz", high["gz"]),
        ]

    def pack_z(values, s, acc):
        here = lax.shift_right_logical(lane, 1) == s
        return tuple(
            jnp.where(here, pltpu.roll(values[x], 2 * s + 1, 1), acc[x]) for x in range(cx)
        )

    def store_z(zs, acc):
        for x in range(cx):
            zs[8 * x : 8 * x + 8, :] = acc[x]

    no_z = (jnp.zeros((8, lanes), F32),) * cx

    loads[0].wait()
    lys[0:cx, :] = lab[pl.ds(0, cx, stride=cy), :]
    lys[cx : 2 * cx, :] = lab[pl.ds(cy - 1, cx, stride=cy), :]
    for copy in loads[1:]:
        copy.wait()
    pl.semaphore_wait(barrier, 2 * len(AXES))
    wave_send()
    first_x = [x_faces(field, xr_b, h) for h in range(CHUNKS)]
    label_copies = [
        ex.start(lab.at[0:8, :], lxr.at[1], "gx", low["gx"]),
        ex.start(lab.at[cells_xy - 8 : cells_xy, :], lxr.at[0], "gx", high["gx"]),
        ex.start(lys, lyr.at[1], "gy", low["gy"]),
        ex.start(lys, lyr.at[0], "gy", high["gy"]),
        ex.start(lab, lzr.at[1], "gz", low["gz"]),
        ex.start(lab, lzr.at[0], "gz", high["gz"]),
    ]
    first_y = []
    for h in range(CHUNKS):
        for s in range(per_chunk * h, per_chunk * (h + 1)):
            for side, y in enumerate((0, cy - 1)):
                ys_b[side, cx * s : cx * s + cx, :] = field[s, pl.ds(y, cx, stride=cy), :]
        first_y.append(y_faces(ys_b, yr_b, h))
    store_z(
        zs_b,
        lax.fori_loop(
            0,
            sensors,
            lambda s, acc: pack_z([field[s, 8 * x : 8 * x + 8, :] for x in range(cx)], s, acc),
            no_z,
            unroll=16,
        ),
    )
    first_z = z_faces(zs_b, zr_b)

    wanted = send_map[...]
    key = lax.shift_right_arithmetic(wanted, 10) * lanes + (wanted & (lanes - 1))
    y_of = lax.shift_right_arithmetic(wanted, 7) & (cy - 1)
    for x in range(cx):
        places = lax.broadcasted_iota(jnp.int32, (lanes, total_slots), 0) + x * lanes
        onehot[x * lanes : (x + 1) * lanes, :] = jnp.where(places == key, 1.0, 0.0).astype(BF16)
    rows_in = lax.broadcasted_iota(jnp.int32, (total_slots, slots.shape[1]), 0)
    slot_cap, slot_y = slots[...] % cap, slots[...] // cap % ny
    slot_row = slot_y * (nx * cap) + slot_cap * nx + slots[...] // (cap * ny)
    pick[...] = jnp.where(rows_in == slot_row, 1.0, 0.0).astype(BF16)
    wave()

    for copy in label_copies:
        copy.wait()

    def tissue(shifted):
        level = jnp.zeros(shifted.shape, F32)
        for k in range(table.shape[0]):
            level = level + jnp.where(shifted == k + 1, table[k], 0.0)
        return level, jnp.where(shifted > 0, 1.0, 0.0).astype(F32)

    shifted = [lab[8 * x : 8 * x + 8, :] + 1 for x in range(cx)]
    for x in range(cx):
        here = shifted[x]
        if x > 0:
            x_low = shifted[x - 1]
        else:
            x_low = jnp.where(has_low["gx"], lxr[0] + 1, 0)
        if x < cx - 1:
            x_high = shifted[x + 1]
        else:
            x_high = jnp.where(has_high["gx"], lxr[1] + 1, 0)
        row_low = jnp.where(has_low["gy"], lyr[0, cx + x : cx + x + 1, :] + 1, 0)
        row_high = jnp.where(has_high["gy"], lyr[1, x : x + 1, :] + 1, 0)
        y_low = jnp.where(row == 0, row_low, pltpu.roll(here, 1, 0))
        y_high = jnp.where(row == cy - 1, row_high, pltpu.roll(here, cy - 1, 0))
        side_low = jnp.where(has_low["gz"], lzr[0, 8 * x : 8 * x + 8, :] + 1, 0)
        side_high = jnp.where(has_high["gz"], lzr[1, 8 * x : 8 * x + 8, :] + 1, 0)
        z_low = pltpu.roll(jnp.where(lane == lanes - 1, side_low, here), 1, 1)
        z_high = pltpu.roll(jnp.where(lane == 0, side_high, here), lanes - 1, 1)
        own_cond, own_in = tissue(here)
        diagonal = jnp.full((8, lanes), MASS, F32)
        for k, beside in enumerate((x_low, x_high, y_low, y_high, z_low, z_high)):
            its_cond, its_in = tissue(beside)
            weight = 0.5 * (own_cond + its_cond) * own_in * its_in
            wts[k, 8 * x : 8 * x + 8, :] = weight
            diagonal = diagonal + weight
        wts[6, 8 * x : 8 * x + 8, :] = diagonal
        wts[7, 8 * x : 8 * x + 8, :] = 0.5 * own_cond
    wave()

    def merge_z(zr):
        for x in range(cx):
            span = slice(8 * x, 8 * x + 8)
            zm[span, :] = jnp.where(
                (lane & 1) == 0,
                pltpu.roll(zr[0, span, :], 2, 1) * keep_low["gz"],
                zr[1, span, :] * keep_high["gz"],
            )

    def neighbours(whole, xr, yr, s, masked):
        own = [whole[s, 8 * x : 8 * x + 8, :] for x in range(cx)]
        outer = [xr[0, s]] + own + [xr[1, s]]
        if masked:
            outer[0], outer[-1] = outer[0] * keep_low["gx"], outer[-1] * keep_high["gx"]
        near = []
        for x in range(cx):
            u = own[x]
            low_row = yr[0, pl.ds(s * cx + x, 1), :]
            high_row = yr[1, pl.ds(s * cx + x, 1), :]
            if masked:
                low_row, high_row = low_row * keep_low["gy"], high_row * keep_high["gy"]
            y_low = jnp.where(row == 0, low_row, pltpu.roll(u, 1, 0))
            y_high = jnp.where(row == cy - 1, high_row, pltpu.roll(u, cy - 1, 0))
            beyond = pltpu.roll(zm[8 * x : 8 * x + 8, :], lanes - 2 - 2 * s, 1)
            z_low = jnp.where(lane == 0, beyond, pltpu.roll(u, 1, 1))
            z_high = jnp.where(lane == lanes - 1, beyond, pltpu.roll(u, lanes - 1, 1))
            near.append((outer[x], outer[x + 2], y_low, y_high, z_low, z_high))
        return own, near

    def apply(own, near, x):
        span = slice(8 * x, 8 * x + 8)
        q = wts[6, span, :] * own[x]
        for n in range(6):
            q = q - wts[n, span, :] * near[x][n]
        return q

    def rows_of(s):
        return pl.ds(pl.multiple_of(8 * s, 8), 8)

    def image_pass(i, acc):
        for k in range(UNROLL):
            s = UNROLL * i + k
            own, near = neighbours(field, xr_b, yr_b, s, False)
            results = [apply(own, near, x) for x in range(cx)]
            for x in range(cx):
                image[s, 8 * x : 8 * x + 8, :] = results[x]
                ys_v[0, pl.ds(s * cx + x, 1), :] = results[x][0:1, :]
                ys_v[1, pl.ds(s * cx + x, 1), :] = results[x][cy - 1 : cy, :]
            acc = pack_z(results, s, acc)
        return acc

    def energy_pass(i, carry):
        for k in range(UNROLL):
            s = UNROLL * i + k
            own, near = neighbours(image, xr_v, yr_v, s, False)
            term = own[0] * apply(own, near, 0)
            for x in range(1, cx):
                term = term + own[x] * apply(own, near, x)
            mq[3, rows_of(s), :] = term
        return carry

    def slope_pass(whole, xr, yr, result, i):
        slopes = [[[None, None] for _ in range(cx)] for _ in range(3)]
        for k in range(2):
            s = 2 * i + k
            own, near = neighbours(whole, xr, yr, s, True)
            sums = [None, None, None]
            for x in range(cx):
                half = wts[7, 8 * x : 8 * x + 8, :]
                for c in range(3):
                    slopes[c][x][k] = half * (near[x][2 * c + 1] - near[x][2 * c])
                if result is not None:
                    q = result[s, 8 * x : 8 * x + 8, :]
                    for n, term in enumerate((own[x] * own[x], own[x] * q, q * q)):
                        sums[n] = term if sums[n] is None else sums[n] + term
            if result is not None:
                for n in range(3):
                    mq[n, rows_of(s), :] = sums[n]
        at = pl.ds(pl.multiple_of(16 * i, 16), 16)
        for c in range(3):
            for x in range(cx):
                slope = jnp.concatenate(slopes[c][x], axis=0)
                coarse = slope.astype(BF16)
                ghi[c, at, x * lanes : (x + 1) * lanes] = coarse
                glo[c, at, x * lanes : (x + 1) * lanes] = (slope - coarse.astype(F32)).astype(BF16)

    def slopes_of(whole, xr, yr, result):
        def step(i, carry):
            for k in range(UNROLL // 2):
                slope_pass(whole, xr, yr, result, UNROLL // 2 * i + k)
            return carry

        lax.fori_loop(0, sensors // UNROLL, step, 0)

    def gather(line):
        parts = []
        for c in range(3):
            product = jnp.dot(ghi[c], onehot[...], preferred_element_type=F32) + jnp.dot(
                glo[c], onehot[...], preferred_element_type=F32
            )
            for h in range(total_slots // lanes):
                raw[h] = product[:, h * lanes : (h + 1) * lanes]
            for g in range(sensors // 8):
                halves = []
                for h in range(total_slots // lanes):
                    acc = None
                    for y in range(cy):
                        strip = raw[h, pl.ds(8 * cy * g + y, 8, stride=cy), :]
                        term = jnp.where(y_of[:, h * lanes : (h + 1) * lanes] == y, strip, 0.0)
                        acc = term if acc is None else acc + term
                    halves.append(acc)
                parts.append(jnp.concatenate(halves, axis=1))
        parts.append(jnp.zeros((lanes - 3 * sensors, total_slots), F32))
        line[...] = jnp.concatenate(parts, axis=0).T

    def spread(source, target, axis):
        rows = source.shape[0] // count[axis]
        mine = pl.ds(pl.multiple_of(me[axis] * rows, rows), rows)
        copies = []
        for d in range(1, count[axis]):
            partner = lax.rem(me[axis] + d, count[axis])
            theirs = pl.ds(pl.multiple_of(partner * rows, rows), rows)
            copies.append(ex.start(source.at[theirs, :], target.at[mine, :], axis, partner))
        target[mine, :] = source[mine, :]
        return copies

    def spread_slabs(source, target, axis):
        mine = me[axis]
        copies = []
        for d in range(1, count[axis]):
            partner = lax.rem(mine + d, count[axis])
            copies.append(ex.start(source.at[partner], target.at[mine], axis, partner))
        target[mine] = source[mine]
        return copies

    tail = lane >= 3 * sensors
    first_rows = row < 4

    def regroup(mid, out):
        for iy in range(ny):
            rows = jnp.concatenate(
                [mid[pl.ds(iy * cap + t, nx, stride=ny * cap), :] for t in range(cap)], axis=0
            )
            for g in range(nx * cap // 16):
                a, b = rows[16 * g : 16 * g + 8, :], rows[16 * g + 8 : 16 * g + 16, :]
                p0 = pltpu.roll(pltpu.roll(b, lanes - sensors, 1), 4, 0)
                p1 = pltpu.roll(b, lanes - 2 * sensors, 1)
                p2 = pltpu.roll(pltpu.roll(b, lanes - 3 * sensors, 1), 4, 0)
                out[iy, 12 * g : 12 * g + 8, :] = jnp.where(tail, jnp.where(first_rows, p0, p1), a)
                out[iy, 12 * g + 8 : 12 * g + 12, :] = jnp.where(tail, p2, b)[0:4, :]

    def unpack(slabs):
        parts = []
        third = lane // sensors
        for iy in range(ny):
            for g in range(nx * cap // 16):
                a = slabs[iy, 12 * g : 12 * g + 8, :]
                b = jnp.concatenate([slabs[iy, 12 * g + 8 : 12 * g + 12, :]] * 2, axis=0)
                p0 = pltpu.roll(pltpu.roll(a, sensors, 1), 4, 0)
                p1 = pltpu.roll(a, 2 * sensors, 1)
                p2 = pltpu.roll(b, 3 * sensors, 1)
                last = jnp.where(third == 0, p0, jnp.where(third == 1, p1, p2))
                parts += [a, jnp.where(first_rows, b, last)]
        return jnp.concatenate(parts, axis=0)

    def reduce_start(buffer, value, partners):
        buffer[0] = value
        return [
            ex.start_at(buffer.at[0], buffer.at[k + 1], where) for k, where in enumerate(partners)
        ]

    def reduce_end(buffer, copies):
        for copy in copies:
            copy.wait()
        value = buffer[0]
        for d in range(1, len(copies) + 1):
            value = value + buffer[d]
        return value

    def moment_rows(m):
        parts = []
        for g in range(sensors // 8):
            acc = None
            for y in range(cy):
                strip = mq[m, pl.ds(8 * cy * g + y, 8, stride=cy), :]
                acc = strip if acc is None else acc + strip
            parts.append(acc)
        return parts

    def lane_sums(parts):
        return lax.dot_general(
            jnp.ones((8, lanes), F32),
            jnp.concatenate(parts, axis=0),
            (((1,), (1,)), ((), ())),
            precision=lax.Precision.HIGHEST,
            preferred_element_type=F32,
        )[0:1, :]

    def select(fin):
        columns = unpack(fin).T
        coarse = columns.astype(BF16)
        fine = (columns - coarse.astype(F32)).astype(BF16)
        return jnp.dot(coarse, pick[...], preferred_element_type=F32) + jnp.dot(
            fine, pick[...], preferred_element_type=F32
        )

    def wait(copies):
        for copy in copies:
            copy.wait()

    blank = [jnp.zeros((8, lanes), F32)]
    steps_per_chunk = per_chunk // UNROLL
    wait(first_z)
    merge_z(zr_b)
    acc = no_z
    second = []
    for h in range(CHUNKS):
        wait(first_x[h] + first_y[h])
        acc = lax.fori_loop(steps_per_chunk * h, steps_per_chunk * (h + 1), image_pass, acc)
        second.append(x_faces(image, xr_v, h) + y_faces(ys_v, yr_v, h))
    store_z(zs_v, acc)
    second_z = z_faces(zs_v, zr_v)
    wave()
    slopes_of(field, xr_b, yr_b, image)
    early = lane_sums(moment_rows(0) + moment_rows(1) + moment_rows(2) + blank * (sensors // 8))
    gather(line_b)
    line_b_copies = spread(line_b, mid_b, "gx")
    wait(second_z)
    merge_z(zr_v)
    for h in range(CHUNKS):
        wait(second[h])
        lax.fori_loop(steps_per_chunk * h, steps_per_chunk * (h + 1), energy_pass, 0)
    partial = early + lane_sums(blank * (3 * sensors // 8) + moment_rows(3))
    wave(len(plan))
    plane = [
        {"gx": lax.rem(me["gx"] + dx, nx), "gz": lax.rem(me["gz"] + dz, nz)}
        for dx in range(nx)
        for dz in range(nz)
        if dx or dz
    ]
    plane_copies = reduce_start(red_plane, partial, plane)
    wait(line_b_copies)
    regroup(mid_b, out_b)
    out_b_copies = spread_slabs(out_b, fin_b, "gy")
    slopes_of(image, xr_v, yr_v, None)
    gather(line_v)
    line_v_copies = spread(line_v, mid_v, "gx")
    line = [{"gy": lax.rem(me["gy"] + d, ny)} for d in range(1, ny)]
    line_copies = reduce_start(red_line, reduce_end(red_plane, plane_copies), line)
    wait(line_v_copies)
    regroup(mid_v, out_v)
    out_v_copies = spread_slabs(out_v, fin_v, "gy")
    wait(out_b_copies)
    owned_b_out[...] = select(fin_b)
    wait(out_v_copies)
    owned_v_out[...] = select(fin_v)
    moments_out[...] = jnp.broadcast_to(reduce_end(red_line, line_copies), (8, lanes))


def finish(moments_in, owned_b, owned_v, data, proj, gram):
    sensors = data.shape[0]
    moments = moments_in[...]
    lanes = moments.shape[1]
    group = lax.broadcasted_iota(jnp.int32, moments.shape, 1) // sensors
    full = []
    for m in range(4):
        value = moments
        for g in range(lanes // sensors):
            shift = (sensors * (g - m)) % lanes
            turn = pltpu.roll(moments, shift, 1) if shift else moments
            value = jnp.where(group == g, turn, value)
        full.append(value)
    zero, one, two, three = full
    first_step = zero / one
    residue = first_step * first_step * two - zero
    growth = 1.0 + residue / zero
    curvature = growth * growth * one - 2.0 * growth * first_step * two + first_step * first_step * three
    second_step = residue / curvature
    source_coef = (first_step + second_step * growth)[0:1, :]
    image_coef = (second_step * first_step)[0:1, :]
    down = (lanes, lanes)
    owned = jnp.broadcast_to(source_coef, down).T * owned_b[...] - jnp.broadcast_to(image_coef, down).T * owned_v[...]
    per_time = data[...].T
    parts = [owned[sensors * c : sensors * (c + 1), :] for c in range(3)]
    for c in range(3):
        proj[c] = jnp.dot(
            per_time, parts[c], precision=lax.Precision.HIGHEST, preferred_element_type=F32
        )
    for k, (a, b) in enumerate(PAIRS):
        gram[k : k + 1, :] = jnp.sum(parts[a] * parts[b], axis=0, keepdims=True)


def per_device(sizes, source_term, labels, table, send_map, owner_slots, sensor_data):
    sensors, cx, cy, lanes = source_term.shape
    cells_xy = cx * cy
    total = send_map.shape[-1]
    owned = owner_slots.shape[0]
    times = sensor_data.shape[1]
    n = copies_needed(sizes)
    vmem = pltpu.VMEM
    scratch = [
        vmem((cells_xy, lanes), jnp.int32),
        pltpu.SMEM(table.shape, F32),
        vmem((1, total), jnp.int32),
        vmem((1, owned), jnp.int32),
        vmem((sensors, cells_xy, lanes), F32),
        vmem((sensors, cells_xy, lanes), F32),
        vmem((2, sensors, 8, lanes), F32),
        vmem((2, sensors, 8, lanes), F32),
        vmem((2, sensors * cx, lanes), F32),
        vmem((2, sensors * cx, lanes), F32),
        vmem((2, sensors * cx, lanes), F32),
        vmem((2, sensors * cx, lanes), F32),
        vmem((cells_xy, lanes), F32),
        vmem((cells_xy, lanes), F32),
        vmem((2, cells_xy, lanes), F32),
        vmem((2, cells_xy, lanes), F32),
        vmem((cells_xy, lanes), F32),
        vmem((2 * cx, lanes), jnp.int32),
        vmem((2, 8, lanes), jnp.int32),
        vmem((2, 2 * cx, lanes), jnp.int32),
        vmem((2, cells_xy, lanes), jnp.int32),
        vmem((8, cells_xy, lanes), F32),
        vmem((3, sensors * 8, cx * lanes), BF16),
        vmem((3, sensors * 8, cx * lanes), BF16),
        vmem((cx * lanes, total), BF16),
        vmem((total, owned), BF16),
        vmem((total // lanes, sensors * 8, lanes), F32),
    ]
    slabs = (sizes[1], total // sizes[1] * 3 // 4, lanes)
    scratch += [vmem((total, lanes), F32)] * 4
    scratch += [vmem(slabs, F32)] * 4
    scratch += [
        vmem((4, sensors * 8, lanes), F32),
        vmem((sizes[0] * sizes[2], 1, lanes), F32),
        vmem((sizes[1], 1, lanes), F32),
        pltpu.SemaphoreType.DMA((4 + CHUNKS,)),
        pltpu.SemaphoreType.DMA((n,)),
        pltpu.SemaphoreType.DMA((n,)),
        pltpu.SemaphoreType.REGULAR((2 * len(AXES) * len(wave_plan(sizes)),)),
    ]
    whole = pl.BlockSpec(memory_space=pltpu.VMEM)
    moments, owned_b, owned_v = pl.pallas_call(
        functools.partial(kernel, sizes),
        out_shape=(
            jax.ShapeDtypeStruct((8, lanes), F32),
            jax.ShapeDtypeStruct((lanes, owned), F32),
            jax.ShapeDtypeStruct((lanes, owned), F32),
        ),
        in_specs=[pl.BlockSpec(memory_space=pltpu.HBM)] * 5,
        out_specs=(whole,) * 3,
        scratch_shapes=scratch,
        compiler_params=pltpu.CompilerParams(
            collective_id=0, has_side_effects=True, vmem_limit_bytes=40 * 1024 * 1024
        ),
        name="solve",
    )(
        *(
            pltpu.with_memory_space_constraint(operand, pltpu.HBM)
            for operand in (
                source_term.reshape(sensors, cells_xy, lanes),
                labels.reshape(cells_xy, lanes),
                table,
                send_map.reshape(1, total),
                owner_slots.reshape(1, owned),
            )
        )
    )
    return pl.pallas_call(
        finish,
        out_shape=(
            jax.ShapeDtypeStruct((3, times, owned), F32),
            jax.ShapeDtypeStruct((len(PAIRS), owned), F32),
        ),
        in_specs=[whole] * 4,
        out_specs=(whole, whole),
        compiler_params=pltpu.CompilerParams(vmem_limit_bytes=40 * 1024 * 1024),
        name="finish",
    )(moments, owned_b, owned_v, sensor_data)


def solution(mesh):
    sizes = tuple(mesh.shape[axis] for axis in AXES)
    in_specs = (
        P(None, "gx", "gy", "gz"),
        P("gx", "gy", "gz"),
        P(),
        P("gx", "gy", "gz", None),
        P(AXES),
        P(),
    )
    out_specs = (P(None, None, AXES), P(None, AXES))
    return jax.shard_map(
        functools.partial(per_device, sizes),
        mesh=mesh,
        in_specs=in_specs,
        out_specs=out_specs,
        check_vma=False,
    )
```

```python
import functools

import jax
import jax.numpy as jnp
from jax import lax
from jax.experimental import pallas as pl
from jax.experimental.pallas import tpu as pltpu
from jax.sharding import PartitionSpec as P

F32 = jnp.float32
BF16 = jnp.bfloat16
MASS = 0.25
PAIRS = ((0, 0), (1, 1), (2, 2), (0, 1), (0, 2), (1, 2))
AXES = ("gx", "gy", "gz")


class Exchange:
    def __init__(self, send, recv):
        self.send, self.recv, self.used = send, recv, 0

    def start(self, source, target, axis, partner):
        return self.start_at(source, target, {axis: partner})

    def start_at(self, source, target, where):
        copy = pltpu.make_async_remote_copy(
            src_ref=source,
            dst_ref=target,
            send_sem=self.send.at[self.used],
            recv_sem=self.recv.at[self.used],
            device_id=where,
            device_id_type=pl.DeviceIdType.MESH,
        )
        self.used += 1
        copy.start()
        return copy


CHUNKS = 2
UNROLL = 8


def copies_needed(sizes):
    nx, ny, nz = sizes
    plane = nx * nz - 1
    return 6 + 2 * (4 * CHUNKS + 2) + plane + 3 * (ny - 1) + 2 * (nx - 1)


def farthest_first(size):
    return sorted(range(1, size), key=lambda d: -min(d, size - d))


def doubling(known, size):
    strides = []
    while known < size // 2:
        strides.append(max(known, 1))
        known += strides[-1]
    return strides


def wave_plan(sizes):
    nx, ny, nz = sizes
    across = [("gx", d) for d in doubling(1, nx)] + [("gz", d) for d in doubling(0, nz)]
    along = [("gy", d) for d in doubling(1, ny)]
    plan = [[] for _ in range(max(len(across), len(along)))]
    for steps in (across, along):
        for k, step in enumerate(steps):
            plan[k].append(step)
    return plan


def kernel(sizes, src, lab_in, table_in, send_in, slots_in, moments_out, owned_b_out, owned_v_out,
           lab, table, send_map, slots, field, image, xr_b, xr_v, ys_b, ys_v, yr_b, yr_v,
           zs_b, zs_v, zr_b, zr_v, zm, lys, lxr, lyr, lzr, wts, ghi, glo, onehot, pick_b, pick_v, raw,
           line_b, line_v, mid_b, mid_v, turn_b, last_b, out_b, out_v, fin_b, fin_v, mq, red_plane, red_line,
           load_sem, send_sem, recv_sem, wave_sem):
    nx, ny, nz = sizes
    count = dict(zip(AXES, sizes))
    me = {axis: lax.axis_index(axis) for axis in AXES}
    low = {axis: lax.rem(me[axis] + count[axis] - 1, count[axis]) for axis in AXES}
    high = {axis: lax.rem(me[axis] + 1, count[axis]) for axis in AXES}
    has_low = {axis: me[axis] > 0 for axis in AXES}
    has_high = {axis: me[axis] < count[axis] - 1 for axis in AXES}
    keep_low = {axis: jnp.where(has_low[axis], 1.0, 0.0).astype(F32) for axis in AXES}
    keep_high = {axis: jnp.where(has_high[axis], 1.0, 0.0).astype(F32) for axis in AXES}
    sensors, cells_xy, lanes = field.shape
    cx, cy = cells_xy // 8, 8
    total_slots = send_map.shape[1]
    cap = total_slots // (nx * ny)
    per_chunk = sensors // CHUNKS
    ex = Exchange(send_sem, recv_sem)
    lane = lax.broadcasted_iota(jnp.int32, (8, lanes), 1)
    row = lax.broadcasted_iota(jnp.int32, (8, lanes), 0)

    def tell(sem, axis, partner):
        pl.semaphore_signal(
            sem, inc=1, device_id={axis: partner}, device_id_type=pl.DeviceIdType.MESH
        )

    loads = [pltpu.make_async_copy(lab_in, lab, load_sem.at[0])]
    for h in range(CHUNKS):
        part = pl.ds(per_chunk * h, per_chunk)
        loads.append(pltpu.make_async_copy(src.at[part], field.at[part], load_sem.at[1 + h]))
    for k, (a, b) in enumerate(((table_in, table), (send_in, send_map), (slots_in, slots))):
        loads.append(pltpu.make_async_copy(a, b, load_sem.at[1 + CHUNKS + k]))
    for copy in loads:
        copy.start()
    barrier = pltpu.get_barrier_semaphore()
    for axis in AXES:
        tell(barrier, axis, low[axis])
        tell(barrier, axis, high[axis])

    plan = wave_plan(sizes)
    wave_at = [0]

    def wave_sems(k, axis):
        first = 2 * (len(AXES) * k + AXES.index(axis))
        return wave_sem.at[first], wave_sem.at[first + 1]

    def wave_send():
        k = wave_at[0]
        if k < len(plan):
            for axis, stride in plan[k]:
                down, up = wave_sems(k, axis)
                tell(down, axis, lax.rem(me[axis] + count[axis] - stride, count[axis]))
                tell(up, axis, lax.rem(me[axis] + stride, count[axis]))

    def wave(times=1):
        for _ in range(times):
            k = wave_at[0]
            if k < len(plan):
                for axis, _stride in plan[k]:
                    for sem in wave_sems(k, axis):
                        pl.semaphore_wait(sem, 1)
                wave_at[0] += 1
                wave_send()

    def x_faces(whole, xr, h):
        part = pl.ds(per_chunk * h, per_chunk)
        last = cells_xy - 8
        return [
            ex.start(whole.at[part, 0:8, :], xr.at[1, part], "gx", low["gx"]),
            ex.start(whole.at[part, last : last + 8, :], xr.at[0, part], "gx", high["gx"]),
        ]

    def y_faces(ys, yr, h):
        part = pl.ds(per_chunk * h * cx, per_chunk * cx)
        return [
            ex.start(ys.at[0, part], yr.at[1, part], "gy", low["gy"]),
            ex.start(ys.at[1, part], yr.at[0, part], "gy", high["gy"]),
        ]

    def z_faces(zs, zr):
        return [
            ex.start(zs, zr.at[1], "gz", low["gz"]),
            ex.start(zs, zr.at[0], "gz", high["gz"]),
        ]

    def pack_z(values, s, acc):
        here = lax.shift_right_logical(lane, 1) == s
        return tuple(
            jnp.where(here, pltpu.roll(values[x], 2 * s + 1, 1), acc[x]) for x in range(cx)
        )

    def store_z(zs, acc):
        for x in range(cx):
            zs[8 * x : 8 * x + 8, :] = acc[x]

    no_z = (jnp.zeros((8, lanes), F32),) * cx

    loads[0].wait()
    lys[0:cx, :] = lab[pl.ds(0, cx, stride=cy), :]
    lys[cx : 2 * cx, :] = lab[pl.ds(cy - 1, cx, stride=cy), :]
    pl.semaphore_wait(barrier, 2 * len(AXES))
    label_copies = [
        ex.start(lab.at[0:8, :], lxr.at[1], "gx", low["gx"]),
        ex.start(lab.at[cells_xy - 8 : cells_xy, :], lxr.at[0], "gx", high["gx"]),
        ex.start(lys, lyr.at[1], "gy", low["gy"]),
        ex.start(lys, lyr.at[0], "gy", high["gy"]),
        ex.start(lab, lzr.at[1], "gz", low["gz"]),
        ex.start(lab, lzr.at[0], "gz", high["gz"]),
    ]
    wave_send()
    first_x = []
    for h in range(CHUNKS):
        loads[1 + h].wait()
        first_x.append(x_faces(field, xr_b, h))
    first_y = []
    for h in range(CHUNKS):
        for s in range(per_chunk * h, per_chunk * (h + 1)):
            for side, y in enumerate((0, cy - 1)):
                ys_b[side, cx * s : cx * s + cx, :] = field[s, pl.ds(y, cx, stride=cy), :]
        first_y.append(y_faces(ys_b, yr_b, h))
    store_z(
        zs_b,
        lax.fori_loop(
            0,
            sensors,
            lambda s, acc: pack_z([field[s, 8 * x : 8 * x + 8, :] for x in range(cx)], s, acc),
            no_z,
            unroll=16,
        ),
    )
    first_z = z_faces(zs_b, zr_b)

    for copy in loads[1 + CHUNKS :]:
        copy.wait()

    wanted = send_map[...]
    key = lax.shift_right_arithmetic(wanted, 10) * lanes + (wanted & (lanes - 1))
    y_of = lax.shift_right_arithmetic(wanted, 7) & (cy - 1)
    for x in range(cx):
        places = lax.broadcasted_iota(jnp.int32, (lanes, total_slots), 0) + x * lanes
        onehot[x * lanes : (x + 1) * lanes, :] = jnp.where(places == key, 1.0, 0.0).astype(BF16)
    rows_in = lax.broadcasted_iota(jnp.int32, (total_slots, slots.shape[1]), 0)
    slot_cap, slot_y = slots[...] % cap, slots[...] // cap % ny
    slot_row = slot_y * (nx * cap) + slot_cap * nx + slots[...] // (cap * ny)
    pick_v[...] = jnp.where(rows_in == slot_row, 1.0, 0.0).astype(BF16)
    pick_b[...] = jnp.where(rows_in == slots[...], 1.0, 0.0).astype(BF16)
    wave()

    for copy in label_copies:
        copy.wait()

    def tissue(shifted):
        level = jnp.zeros(shifted.shape, F32)
        for k in range(table.shape[0]):
            level = level + jnp.where(shifted == k + 1, table[k], 0.0)
        return level, jnp.where(shifted > 0, 1.0, 0.0).astype(F32)

    shifted = [lab[8 * x : 8 * x + 8, :] + 1 for x in range(cx)]
    for x in range(cx):
        here = shifted[x]
        if x > 0:
            x_low = shifted[x - 1]
        else:
            x_low = jnp.where(has_low["gx"], lxr[0] + 1, 0)
        if x < cx - 1:
            x_high = shifted[x + 1]
        else:
            x_high = jnp.where(has_high["gx"], lxr[1] + 1, 0)
        row_low = jnp.where(has_low["gy"], lyr[0, cx + x : cx + x + 1, :] + 1, 0)
        row_high = jnp.where(has_high["gy"], lyr[1, x : x + 1, :] + 1, 0)
        y_low = jnp.where(row == 0, row_low, pltpu.roll(here, 1, 0))
        y_high = jnp.where(row == cy - 1, row_high, pltpu.roll(here, cy - 1, 0))
        side_low = jnp.where(has_low["gz"], lzr[0, 8 * x : 8 * x + 8, :] + 1, 0)
        side_high = jnp.where(has_high["gz"], lzr[1, 8 * x : 8 * x + 8, :] + 1, 0)
        z_low = pltpu.roll(jnp.where(lane == lanes - 1, side_low, here), 1, 1)
        z_high = pltpu.roll(jnp.where(lane == 0, side_high, here), lanes - 1, 1)
        own_cond, own_in = tissue(here)
        diagonal = jnp.full((8, lanes), MASS, F32)
        for k, beside in enumerate((x_low, x_high, y_low, y_high, z_low, z_high)):
            its_cond, its_in = tissue(beside)
            weight = 0.5 * (own_cond + its_cond) * own_in * its_in
            wts[k, 8 * x : 8 * x + 8, :] = weight
            diagonal = diagonal + weight
        wts[6, 8 * x : 8 * x + 8, :] = diagonal
        wts[7, 8 * x : 8 * x + 8, :] = 0.5 * own_cond
    wave()

    def merge_z(zr):
        for x in range(cx):
            span = slice(8 * x, 8 * x + 8)
            zm[span, :] = jnp.where(
                (lane & 1) == 0,
                pltpu.roll(zr[0, span, :], 2, 1) * keep_low["gz"],
                zr[1, span, :] * keep_high["gz"],
            )

    def neighbours(whole, xr, yr, s, masked):
        own = [whole[s, 8 * x : 8 * x + 8, :] for x in range(cx)]
        outer = [xr[0, s]] + own + [xr[1, s]]
        if masked:
            outer[0], outer[-1] = outer[0] * keep_low["gx"], outer[-1] * keep_high["gx"]
        near = []
        for x in range(cx):
            u = own[x]
            low_row = yr[0, pl.ds(s * cx + x, 1), :]
            high_row = yr[1, pl.ds(s * cx + x, 1), :]
            if masked:
                low_row, high_row = low_row * keep_low["gy"], high_row * keep_high["gy"]
            y_low = jnp.where(row == 0, low_row, pltpu.roll(u, 1, 0))
            y_high = jnp.where(row == cy - 1, high_row, pltpu.roll(u, cy - 1, 0))
            beyond = pltpu.roll(zm[8 * x : 8 * x + 8, :], lanes - 2 - 2 * s, 1)
            z_low = jnp.where(lane == 0, beyond, pltpu.roll(u, 1, 1))
            z_high = jnp.where(lane == lanes - 1, beyond, pltpu.roll(u, lanes - 1, 1))
            near.append((outer[x], outer[x + 2], y_low, y_high, z_low, z_high))
        return own, near

    def apply(own, near, x):
        span = slice(8 * x, 8 * x + 8)
        q = wts[6, span, :] * own[x]
        for n in range(6):
            q = q - wts[n, span, :] * near[x][n]
        return q

    def rows_of(s):
        return pl.ds(pl.multiple_of(8 * s, 8), 8)

    def image_pass(i, acc):
        for k in range(UNROLL):
            s = UNROLL * i + k
            own, near = neighbours(field, xr_b, yr_b, s, False)
            results = [apply(own, near, x) for x in range(cx)]
            for x in range(cx):
                image[s, 8 * x : 8 * x + 8, :] = results[x]
                ys_v[0, pl.ds(s * cx + x, 1), :] = results[x][0:1, :]
                ys_v[1, pl.ds(s * cx + x, 1), :] = results[x][cy - 1 : cy, :]
            acc = pack_z(results, s, acc)
        return acc

    def energy_pass(i, carry):
        for k in range(UNROLL):
            s = UNROLL * i + k
            own, near = neighbours(image, xr_v, yr_v, s, False)
            term = own[0] * apply(own, near, 0)
            for x in range(1, cx):
                term = term + own[x] * apply(own, near, x)
            mq[3, rows_of(s), :] = term
        return carry

    def slope_pass(whole, xr, yr, result, i):
        slopes = [[[None, None] for _ in range(cx)] for _ in range(3)]
        for k in range(2):
            s = 2 * i + k
            own, near = neighbours(whole, xr, yr, s, True)
            sums = [None, None, None]
            for x in range(cx):
                half = wts[7, 8 * x : 8 * x + 8, :]
                for c in range(3):
                    slopes[c][x][k] = half * (near[x][2 * c + 1] - near[x][2 * c])
                if result is not None:
                    q = result[s, 8 * x : 8 * x + 8, :]
                    for n, term in enumerate((own[x] * own[x], own[x] * q, q * q)):
                        sums[n] = term if sums[n] is None else sums[n] + term
            if result is not None:
                for n in range(3):
                    mq[n, rows_of(s), :] = sums[n]
        at = pl.ds(pl.multiple_of(16 * i, 16), 16)
        for c in range(3):
            for x in range(cx):
                slope = jnp.concatenate(slopes[c][x], axis=0)
                coarse = slope.astype(BF16)
                ghi[c, at, x * lanes : (x + 1) * lanes] = coarse
                glo[c, at, x * lanes : (x + 1) * lanes] = (slope - coarse.astype(F32)).astype(BF16)

    def slopes_of(whole, xr, yr, result):
        def step(i, carry):
            for k in range(UNROLL // 2):
                slope_pass(whole, xr, yr, result, UNROLL // 2 * i + k)
            return carry

        lax.fori_loop(0, sensors // UNROLL, step, 0)

    def gather(line):
        parts = []
        for c in range(3):
            product = jnp.dot(ghi[c], onehot[...], preferred_element_type=F32) + jnp.dot(
                glo[c], onehot[...], preferred_element_type=F32
            )
            for h in range(total_slots // lanes):
                raw[h] = product[:, h * lanes : (h + 1) * lanes]
            for g in range(sensors // 8):
                halves = []
                for h in range(total_slots // lanes):
                    acc = None
                    for y in range(cy):
                        strip = raw[h, pl.ds(8 * cy * g + y, 8, stride=cy), :]
                        term = jnp.where(y_of[:, h * lanes : (h + 1) * lanes] == y, strip, 0.0)
                        acc = term if acc is None else acc + term
                    halves.append(acc)
                parts.append(jnp.concatenate(halves, axis=1))
        parts.append(jnp.zeros((lanes - 3 * sensors, total_slots), F32))
        line[...] = jnp.concatenate(parts, axis=0).T

    def spread(source, target, axis):
        rows = source.shape[0] // count[axis]
        mine = pl.ds(pl.multiple_of(me[axis] * rows, rows), rows)
        copies = []
        for d in farthest_first(count[axis]):
            partner = lax.rem(me[axis] + d, count[axis])
            theirs = pl.ds(pl.multiple_of(partner * rows, rows), rows)
            copies.append(ex.start(source.at[theirs, :], target.at[mine, :], axis, partner))
        target[mine, :] = source[mine, :]
        return copies

    def spread_slabs(source, target, axis):
        mine = me[axis]
        copies = []
        for d in farthest_first(count[axis]):
            partner = lax.rem(mine + d, count[axis])
            copies.append(ex.start(source.at[partner], target.at[mine], axis, partner))
        target[mine] = source[mine]
        return copies

    tail = lane >= 3 * sensors
    first_rows = row < 4

    def regroup(mid, out):
        for iy in range(ny):
            rows = jnp.concatenate(
                [mid[pl.ds(iy * cap + t, nx, stride=ny * cap), :] for t in range(cap)], axis=0
            )
            for g in range(nx * cap // 16):
                a, b = rows[16 * g : 16 * g + 8, :], rows[16 * g + 8 : 16 * g + 16, :]
                p0 = pltpu.roll(pltpu.roll(b, lanes - sensors, 1), 4, 0)
                p1 = pltpu.roll(b, lanes - 2 * sensors, 1)
                p2 = pltpu.roll(pltpu.roll(b, lanes - 3 * sensors, 1), 4, 0)
                out[iy, 12 * g : 12 * g + 8, :] = jnp.where(tail, jnp.where(first_rows, p0, p1), a)
                out[iy, 12 * g + 8 : 12 * g + 12, :] = jnp.where(tail, p2, b)[0:4, :]

    def unpack(slabs):
        parts = []
        third = lane // sensors
        for iy in range(ny):
            for g in range(nx * cap // 16):
                a = slabs[iy, 12 * g : 12 * g + 8, :]
                b = jnp.concatenate([slabs[iy, 12 * g + 8 : 12 * g + 12, :]] * 2, axis=0)
                p0 = pltpu.roll(pltpu.roll(a, sensors, 1), 4, 0)
                p1 = pltpu.roll(a, 2 * sensors, 1)
                p2 = pltpu.roll(b, 3 * sensors, 1)
                last = jnp.where(third == 0, p0, jnp.where(third == 1, p1, p2))
                parts += [a, jnp.where(first_rows, b, last)]
        return jnp.concatenate(parts, axis=0)

    def reduce_start(buffer, value, partners):
        buffer[0] = value
        return [
            ex.start_at(buffer.at[0], buffer.at[k + 1], where) for k, where in enumerate(partners)
        ]

    def reduce_end(buffer, copies):
        for copy in copies:
            copy.wait()
        value = buffer[0]
        for d in range(1, len(copies) + 1):
            value = value + buffer[d]
        return value

    def moment_rows(m):
        parts = []
        for g in range(sensors // 8):
            acc = None
            for y in range(cy):
                strip = mq[m, pl.ds(8 * cy * g + y, 8, stride=cy), :]
                acc = strip if acc is None else acc + strip
            parts.append(acc)
        return parts

    def lane_sums(parts):
        return lax.dot_general(
            jnp.ones((8, lanes), F32),
            jnp.concatenate(parts, axis=0),
            (((1,), (1,)), ((), ())),
            precision=lax.Precision.HIGHEST,
            preferred_element_type=F32,
        )[0:1, :]

    def select(rows, pick):
        columns = rows.T
        coarse = columns.astype(BF16)
        fine = (columns - coarse.astype(F32)).astype(BF16)
        return jnp.dot(coarse, pick[...], preferred_element_type=F32) + jnp.dot(
            fine, pick[...], preferred_element_type=F32
        )

    def wait(copies):
        for copy in copies:
            copy.wait()

    blank = [jnp.zeros((8, lanes), F32)]
    steps_per_chunk = per_chunk // UNROLL
    wait(first_z)
    merge_z(zr_b)
    acc = no_z
    second = []
    for h in range(CHUNKS):
        wait(first_x[h] + first_y[h])
        acc = lax.fori_loop(steps_per_chunk * h, steps_per_chunk * (h + 1), image_pass, acc)
        second.append(x_faces(image, xr_v, h) + y_faces(ys_v, yr_v, h))
    store_z(zs_v, acc)
    second_z = z_faces(zs_v, zr_v)
    wave()
    slopes_of(field, xr_b, yr_b, image)
    early = lane_sums(moment_rows(0) + moment_rows(1) + moment_rows(2) + blank * (sensors // 8))
    gather(line_b)
    regroup(line_b, out_b)
    wave(len(plan))
    out_b_copies = spread_slabs(out_b, fin_b, "gy")
    wait(second_z)
    merge_z(zr_v)
    for h in range(CHUNKS):
        wait(second[h])
        lax.fori_loop(steps_per_chunk * h, steps_per_chunk * (h + 1), energy_pass, 0)
    partial = early + lane_sums(blank * (3 * sensors // 8) + moment_rows(3))
    plane = [
        {"gx": lax.rem(me["gx"] + dx, nx), "gz": lax.rem(me["gz"] + dz, nz)}
        for dx in farthest_first(nx) + [0]
        for dz in farthest_first(nz) + [0]
        if dx or dz
    ]
    plane_copies = reduce_start(red_plane, partial, plane)
    slopes_of(image, xr_v, yr_v, None)
    gather(line_v)
    line_v_copies = spread(line_v, mid_v, "gx")
    line = [{"gy": lax.rem(me["gy"] + d, ny)} for d in farthest_first(ny)]
    line_copies = reduce_start(red_line, reduce_end(red_plane, plane_copies), line)
    wait(line_v_copies)
    regroup(mid_v, out_v)
    out_v_copies = spread_slabs(out_v, fin_v, "gy")
    wait(out_b_copies)
    mid_b[...] = unpack(fin_b)
    for ix in range(nx):
        turn_b[ix * ny * cap : (ix + 1) * ny * cap, :] = mid_b[pl.ds(ix, ny * cap, stride=nx), :]
    last_b_copies = spread(turn_b, last_b, "gx")
    wait(last_b_copies)
    owned_b_out[...] = select(last_b[...], pick_b)
    wait(out_v_copies)
    owned_v_out[...] = select(unpack(fin_v), pick_v)
    moments_out[...] = jnp.broadcast_to(reduce_end(red_line, line_copies), (8, lanes))


def finish(moments_in, owned_b, owned_v, data, proj, gram):
    sensors = data.shape[0]
    moments = moments_in[...]
    lanes = moments.shape[1]
    group = lax.broadcasted_iota(jnp.int32, moments.shape, 1) // sensors
    full = []
    for m in range(4):
        value = moments
        for g in range(lanes // sensors):
            shift = (sensors * (g - m)) % lanes
            turn = pltpu.roll(moments, shift, 1) if shift else moments
            value = jnp.where(group == g, turn, value)
        full.append(value)
    zero, one, two, three = full
    first_step = zero / one
    residue = first_step * first_step * two - zero
    growth = 1.0 + residue / zero
    curvature = growth * growth * one - 2.0 * growth * first_step * two + first_step * first_step * three
    second_step = residue / curvature
    source_coef = (first_step + second_step * growth)[0:1, :]
    image_coef = (second_step * first_step)[0:1, :]
    down = (lanes, lanes)
    owned = jnp.broadcast_to(source_coef, down).T * owned_b[...] - jnp.broadcast_to(image_coef, down).T * owned_v[...]
    per_time = data[...].T
    parts = [owned[sensors * c : sensors * (c + 1), :] for c in range(3)]
    for c in range(3):
        proj[c] = jnp.dot(
            per_time, parts[c], precision=lax.Precision.HIGHEST, preferred_element_type=F32
        )
    for k, (a, b) in enumerate(PAIRS):
        gram[k : k + 1, :] = jnp.sum(parts[a] * parts[b], axis=0, keepdims=True)


def per_device(sizes, source_term, labels, table, send_map, owner_slots, sensor_data):
    sensors, cx, cy, lanes = source_term.shape
    cells_xy = cx * cy
    total = send_map.shape[-1]
    owned = owner_slots.shape[0]
    times = sensor_data.shape[1]
    n = copies_needed(sizes)
    vmem = pltpu.VMEM
    scratch = [
        vmem((cells_xy, lanes), jnp.int32),
        pltpu.SMEM(table.shape, F32),
        vmem((1, total), jnp.int32),
        vmem((1, owned), jnp.int32),
        vmem((sensors, cells_xy, lanes), F32),
        vmem((sensors, cells_xy, lanes), F32),
        vmem((2, sensors, 8, lanes), F32),
        vmem((2, sensors, 8, lanes), F32),
        vmem((2, sensors * cx, lanes), F32),
        vmem((2, sensors * cx, lanes), F32),
        vmem((2, sensors * cx, lanes), F32),
        vmem((2, sensors * cx, lanes), F32),
        vmem((cells_xy, lanes), F32),
        vmem((cells_xy, lanes), F32),
        vmem((2, cells_xy, lanes), F32),
        vmem((2, cells_xy, lanes), F32),
        vmem((cells_xy, lanes), F32),
        vmem((2 * cx, lanes), jnp.int32),
        vmem((2, 8, lanes), jnp.int32),
        vmem((2, 2 * cx, lanes), jnp.int32),
        vmem((2, cells_xy, lanes), jnp.int32),
        vmem((8, cells_xy, lanes), F32),
        vmem((3, sensors * 8, cx * lanes), BF16),
        vmem((3, sensors * 8, cx * lanes), BF16),
        vmem((cx * lanes, total), BF16),
        vmem((total, owned), BF16),
        vmem((total, owned), BF16),
        vmem((total // lanes, sensors * 8, lanes), F32),
    ]
    slabs = (sizes[1], total // sizes[1] * 3 // 4, lanes)
    scratch += [vmem((total, lanes), F32)] * 6
    scratch += [vmem(slabs, F32)] * 4
    scratch += [
        vmem((4, sensors * 8, lanes), F32),
        vmem((sizes[0] * sizes[2], 1, lanes), F32),
        vmem((sizes[1], 1, lanes), F32),
        pltpu.SemaphoreType.DMA((4 + CHUNKS,)),
        pltpu.SemaphoreType.DMA((n,)),
        pltpu.SemaphoreType.DMA((n,)),
        pltpu.SemaphoreType.REGULAR((2 * len(AXES) * len(wave_plan(sizes)),)),
    ]
    whole = pl.BlockSpec(memory_space=pltpu.VMEM)
    moments, owned_b, owned_v = pl.pallas_call(
        functools.partial(kernel, sizes),
        out_shape=(
            jax.ShapeDtypeStruct((8, lanes), F32),
            jax.ShapeDtypeStruct((lanes, owned), F32),
            jax.ShapeDtypeStruct((lanes, owned), F32),
        ),
        in_specs=[pl.BlockSpec(memory_space=pltpu.HBM)] * 5,
        out_specs=(whole,) * 3,
        scratch_shapes=scratch,
        compiler_params=pltpu.CompilerParams(
            collective_id=0, has_side_effects=True, vmem_limit_bytes=40 * 1024 * 1024
        ),
        name="solve",
    )(
        *(
            pltpu.with_memory_space_constraint(operand, pltpu.HBM)
            for operand in (
                source_term.reshape(sensors, cells_xy, lanes),
                labels.reshape(cells_xy, lanes),
                table,
                send_map.reshape(1, total),
                owner_slots.reshape(1, owned),
            )
        )
    )
    return pl.pallas_call(
        finish,
        out_shape=(
            jax.ShapeDtypeStruct((3, times, owned), F32),
            jax.ShapeDtypeStruct((len(PAIRS), owned), F32),
        ),
        in_specs=[whole] * 4,
        out_specs=(whole, whole),
        compiler_params=pltpu.CompilerParams(vmem_limit_bytes=40 * 1024 * 1024),
        name="finish",
    )(moments, owned_b, owned_v, sensor_data)


def solution(mesh):
    sizes = tuple(mesh.shape[axis] for axis in AXES)
    in_specs = (
        P(None, "gx", "gy", "gz"),
        P("gx", "gy", "gz"),
        P(),
        P("gx", "gy", "gz", None),
        P(AXES),
        P(),
    )
    out_specs = (P(None, None, AXES), P(None, AXES))
    return jax.shard_map(
        functools.partial(per_device, sizes),
        mesh=mesh,
        in_specs=in_specs,
        out_specs=out_specs,
        check_vma=False,
    )
```

```python
import functools

import jax
import jax.numpy as jnp
from jax import lax
from jax.experimental import pallas as pl
from jax.experimental.pallas import tpu as pltpu
from jax.sharding import PartitionSpec as P

F32 = jnp.float32
BF16 = jnp.bfloat16
MASS = 0.25
PAIRS = ((0, 0), (1, 1), (2, 2), (0, 1), (0, 2), (1, 2))
AXES = ("gx", "gy", "gz")


class Exchange:
    def __init__(self, send, recv):
        self.send, self.recv, self.used = send, recv, 0

    def copy(self, source, target, where):
        return pltpu.make_async_remote_copy(
            src_ref=source,
            dst_ref=target,
            send_sem=self.send.at[self.used],
            recv_sem=self.recv.at[self.used],
            device_id=where,
            device_id_type=pl.DeviceIdType.MESH,
        )

    def start(self, copies, arrived):
        for source, target, where in copies:
            self.copy(source, target, where).start()
        whole = self.copy(arrived, arrived, copies[0][2])
        self.used += 1
        return whole


CHUNKS = 2
UNROLL = 8


GROUPS = 3 + 2 * (2 * CHUNKS + 1) + 4 + 2


def farthest_first(size):
    return sorted(range(1, size), key=lambda d: -min(d, size - d))


def doubling(known, size):
    strides = []
    while known < size // 2:
        strides.append(max(known, 1))
        known += strides[-1]
    return strides


def wave_plan(sizes):
    nx, ny, nz = sizes
    across = [("gx", d) for d in doubling(1, nx)] + [("gz", d) for d in doubling(0, nz)]
    along = [("gy", d) for d in doubling(1, ny)]
    plan = [[] for _ in range(max(len(across), len(along)))]
    for steps in (across, along):
        for k, step in enumerate(steps):
            plan[k].append(step)
    return plan


def kernel(sizes, src, lab_in, table_in, send_in, slots_in, moments_out, owned_b_out, owned_v_out,
           lab, table, send_map, slots, field, image, xr_b, xr_v, ys_b, ys_v, yr_b, yr_v,
           zs_b, zs_v, zr_b, zr_v, zm, lys, lxr, lyr, lzr, wts, ghi, glo, onehot, pick_b, pick_v, raw,
           line_b, line_v, mid_b, mid_v, turn_b, last_b, out_b, out_v, fin_b, fin_v, mq, red_plane, red_line,
           load_sem, send_sem, recv_sem, wave_sem):
    nx, ny, nz = sizes
    count = dict(zip(AXES, sizes))
    me = {axis: lax.axis_index(axis) for axis in AXES}
    low = {axis: lax.rem(me[axis] + count[axis] - 1, count[axis]) for axis in AXES}
    high = {axis: lax.rem(me[axis] + 1, count[axis]) for axis in AXES}
    has_low = {axis: me[axis] > 0 for axis in AXES}
    has_high = {axis: me[axis] < count[axis] - 1 for axis in AXES}
    keep_low = {axis: jnp.where(has_low[axis], 1.0, 0.0).astype(F32) for axis in AXES}
    keep_high = {axis: jnp.where(has_high[axis], 1.0, 0.0).astype(F32) for axis in AXES}
    sensors, cells_xy, lanes = field.shape
    cx, cy = cells_xy // 8, 8
    total_slots = send_map.shape[1]
    cap = total_slots // (nx * ny)
    per_chunk = sensors // CHUNKS
    ex = Exchange(send_sem, recv_sem)
    lane = lax.broadcasted_iota(jnp.int32, (8, lanes), 1)
    row = lax.broadcasted_iota(jnp.int32, (8, lanes), 0)

    def tell(sem, axis, partner):
        pl.semaphore_signal(
            sem, inc=1, device_id={axis: partner}, device_id_type=pl.DeviceIdType.MESH
        )

    loads = [pltpu.make_async_copy(lab_in, lab, load_sem.at[0])]
    for h in range(CHUNKS):
        part = pl.ds(per_chunk * h, per_chunk)
        loads.append(pltpu.make_async_copy(src.at[part], field.at[part], load_sem.at[1 + h]))
    for k, (a, b) in enumerate(((table_in, table), (send_in, send_map), (slots_in, slots))):
        loads.append(pltpu.make_async_copy(a, b, load_sem.at[1 + CHUNKS + k]))
    for copy in loads:
        copy.start()
    barrier = pltpu.get_barrier_semaphore()
    for axis in AXES:
        tell(barrier, axis, low[axis])
        tell(barrier, axis, high[axis])

    plan = wave_plan(sizes)
    wave_at = [0]

    def wave_sems(k, axis):
        return wave_sem.at[len(AXES) * k + AXES.index(axis)]

    def wave_send():
        k = wave_at[0]
        if k < len(plan):
            for axis, stride in plan[k]:
                sem = wave_sems(k, axis)
                tell(sem, axis, lax.rem(me[axis] + count[axis] - stride, count[axis]))
                tell(sem, axis, lax.rem(me[axis] + stride, count[axis]))

    def wave(times=1):
        for _ in range(times):
            k = wave_at[0]
            if k < len(plan):
                for axis, _stride in plan[k]:
                    pl.semaphore_wait(wave_sems(k, axis), 2)
                wave_at[0] += 1
                wave_send()

    def both_ways(to_low, to_high, target, arrived, axis):
        copies = (
            (to_low, target(1), {axis: low[axis]}),
            (to_high, target(0), {axis: high[axis]}),
        )
        return [ex.start(copies, arrived)]

    def x_faces(whole, xr, h):
        part = pl.ds(per_chunk * h, per_chunk)
        last = cells_xy - 8
        return both_ways(
            whole.at[part, 0:8, :],
            whole.at[part, last : last + 8, :],
            lambda side: xr.at[side, part],
            xr.at[:, part],
            "gx",
        )

    def y_faces(ys, yr, h):
        part = pl.ds(per_chunk * h * cx, per_chunk * cx)
        return both_ways(
            ys.at[0, part], ys.at[1, part], lambda side: yr.at[side, part], yr.at[:, part], "gy"
        )

    def z_faces(zs, zr):
        return both_ways(zs, zs, lambda side: zr.at[side], zr, "gz")

    def pack_z(values, s, acc):
        here = lax.shift_right_logical(lane, 1) == s
        return tuple(
            jnp.where(here, pltpu.roll(values[x], 2 * s + 1, 1), acc[x]) for x in range(cx)
        )

    def store_z(zs, acc):
        for x in range(cx):
            zs[8 * x : 8 * x + 8, :] = acc[x]

    no_z = (jnp.zeros((8, lanes), F32),) * cx

    loads[0].wait()
    lys[0:cx, :] = lab[pl.ds(0, cx, stride=cy), :]
    lys[cx : 2 * cx, :] = lab[pl.ds(cy - 1, cx, stride=cy), :]
    pl.semaphore_wait(barrier, 2 * len(AXES))
    label_copies = (
        both_ways(lab.at[0:8, :], lab.at[cells_xy - 8 : cells_xy, :], lambda side: lxr.at[side], lxr, "gx")
        + both_ways(lys, lys, lambda side: lyr.at[side], lyr, "gy")
        + both_ways(lab, lab, lambda side: lzr.at[side], lzr, "gz")
    )
    wave_send()
    first_x = []
    for h in range(CHUNKS):
        loads[1 + h].wait()
        first_x.append(x_faces(field, xr_b, h))
    first_y = []
    for h in range(CHUNKS):
        for s in range(per_chunk * h, per_chunk * (h + 1)):
            for side, y in enumerate((0, cy - 1)):
                ys_b[side, cx * s : cx * s + cx, :] = field[s, pl.ds(y, cx, stride=cy), :]
        first_y.append(y_faces(ys_b, yr_b, h))
    store_z(
        zs_b,
        lax.fori_loop(
            0,
            sensors,
            lambda s, acc: pack_z([field[s, 8 * x : 8 * x + 8, :] for x in range(cx)], s, acc),
            no_z,
            unroll=16,
        ),
    )
    first_z = z_faces(zs_b, zr_b)

    for copy in loads[1 + CHUNKS :]:
        copy.wait()

    wanted = send_map[...]
    key = lax.shift_right_arithmetic(wanted, 10) * lanes + (wanted & (lanes - 1))
    y_of = lax.shift_right_arithmetic(wanted, 7) & (cy - 1)
    for x in range(cx):
        places = lax.broadcasted_iota(jnp.int32, (lanes, total_slots), 0) + x * lanes
        onehot[x * lanes : (x + 1) * lanes, :] = jnp.where(places == key, 1.0, 0.0).astype(BF16)
    rows_in = lax.broadcasted_iota(jnp.int32, (total_slots, slots.shape[1]), 0)
    slot_cap, slot_y = slots[...] % cap, slots[...] // cap % ny
    slot_row = slot_y * (nx * cap) + slot_cap * nx + slots[...] // (cap * ny)
    pick_v[...] = jnp.where(rows_in == slot_row, 1.0, 0.0).astype(BF16)
    pick_b[...] = jnp.where(rows_in == slots[...], 1.0, 0.0).astype(BF16)
    wave()

    for copy in label_copies:
        copy.wait()

    def tissue(shifted):
        level = jnp.zeros(shifted.shape, F32)
        for k in range(table.shape[0]):
            level = level + jnp.where(shifted == k + 1, table[k], 0.0)
        return level, jnp.where(shifted > 0, 1.0, 0.0).astype(F32)

    shifted = [lab[8 * x : 8 * x + 8, :] + 1 for x in range(cx)]
    for x in range(cx):
        here = shifted[x]
        if x > 0:
            x_low = shifted[x - 1]
        else:
            x_low = jnp.where(has_low["gx"], lxr[0] + 1, 0)
        if x < cx - 1:
            x_high = shifted[x + 1]
        else:
            x_high = jnp.where(has_high["gx"], lxr[1] + 1, 0)
        row_low = jnp.where(has_low["gy"], lyr[0, cx + x : cx + x + 1, :] + 1, 0)
        row_high = jnp.where(has_high["gy"], lyr[1, x : x + 1, :] + 1, 0)
        y_low = jnp.where(row == 0, row_low, pltpu.roll(here, 1, 0))
        y_high = jnp.where(row == cy - 1, row_high, pltpu.roll(here, cy - 1, 0))
        side_low = jnp.where(has_low["gz"], lzr[0, 8 * x : 8 * x + 8, :] + 1, 0)
        side_high = jnp.where(has_high["gz"], lzr[1, 8 * x : 8 * x + 8, :] + 1, 0)
        z_low = pltpu.roll(jnp.where(lane == lanes - 1, side_low, here), 1, 1)
        z_high = pltpu.roll(jnp.where(lane == 0, side_high, here), lanes - 1, 1)
        own_cond, own_in = tissue(here)
        diagonal = jnp.full((8, lanes), MASS, F32)
        for k, beside in enumerate((x_low, x_high, y_low, y_high, z_low, z_high)):
            its_cond, its_in = tissue(beside)
            weight = 0.5 * (own_cond + its_cond) * own_in * its_in
            wts[k, 8 * x : 8 * x + 8, :] = weight
            diagonal = diagonal + weight
        wts[6, 8 * x : 8 * x + 8, :] = diagonal
        wts[7, 8 * x : 8 * x + 8, :] = 0.5 * own_cond
    wave()

    def merge_z(zr):
        for x in range(cx):
            span = slice(8 * x, 8 * x + 8)
            zm[span, :] = jnp.where(
                (lane & 1) == 0,
                pltpu.roll(zr[0, span, :], 2, 1) * keep_low["gz"],
                zr[1, span, :] * keep_high["gz"],
            )

    def neighbours(whole, xr, yr, s, masked):
        own = [whole[s, 8 * x : 8 * x + 8, :] for x in range(cx)]
        outer = [xr[0, s]] + own + [xr[1, s]]
        if masked:
            outer[0], outer[-1] = outer[0] * keep_low["gx"], outer[-1] * keep_high["gx"]
        near = []
        for x in range(cx):
            u = own[x]
            low_row = yr[0, pl.ds(s * cx + x, 1), :]
            high_row = yr[1, pl.ds(s * cx + x, 1), :]
            if masked:
                low_row, high_row = low_row * keep_low["gy"], high_row * keep_high["gy"]
            y_low = jnp.where(row == 0, low_row, pltpu.roll(u, 1, 0))
            y_high = jnp.where(row == cy - 1, high_row, pltpu.roll(u, cy - 1, 0))
            beyond = pltpu.roll(zm[8 * x : 8 * x + 8, :], lanes - 2 - 2 * s, 1)
            z_low = jnp.where(lane == 0, beyond, pltpu.roll(u, 1, 1))
            z_high = jnp.where(lane == lanes - 1, beyond, pltpu.roll(u, lanes - 1, 1))
            near.append((outer[x], outer[x + 2], y_low, y_high, z_low, z_high))
        return own, near

    def apply(own, near, x):
        span = slice(8 * x, 8 * x + 8)
        q = wts[6, span, :] * own[x]
        for n in range(6):
            q = q - wts[n, span, :] * near[x][n]
        return q

    def rows_of(s):
        return pl.ds(pl.multiple_of(8 * s, 8), 8)

    def image_pass(i, acc):
        for k in range(UNROLL):
            s = UNROLL * i + k
            own, near = neighbours(field, xr_b, yr_b, s, False)
            results = [apply(own, near, x) for x in range(cx)]
            for x in range(cx):
                image[s, 8 * x : 8 * x + 8, :] = results[x]
                ys_v[0, pl.ds(s * cx + x, 1), :] = results[x][0:1, :]
                ys_v[1, pl.ds(s * cx + x, 1), :] = results[x][cy - 1 : cy, :]
            acc = pack_z(results, s, acc)
        return acc

    def slope_pass(whole, xr, yr, result, i):
        slopes = [[[None, None] for _ in range(cx)] for _ in range(3)]
        for k in range(2):
            s = 2 * i + k
            own, near = neighbours(whole, xr, yr, s, True)
            sums = [None, None, None]
            for x in range(cx):
                half = wts[7, 8 * x : 8 * x + 8, :]
                for c in range(3):
                    slopes[c][x][k] = half * (near[x][2 * c + 1] - near[x][2 * c])
                if result is not None:
                    q = result[s, 8 * x : 8 * x + 8, :]
                    for n, term in enumerate((own[x] * own[x], own[x] * q, q * q)):
                        sums[n] = term if sums[n] is None else sums[n] + term
                else:
                    term = own[x] * apply(own, near, x)
                    sums[0] = term if sums[0] is None else sums[0] + term
            if result is not None:
                for n in range(3):
                    mq[n, rows_of(s), :] = sums[n]
            else:
                mq[3, rows_of(s), :] = sums[0]
        at = pl.ds(pl.multiple_of(16 * i, 16), 16)
        for c in range(3):
            for x in range(cx):
                slope = jnp.concatenate(slopes[c][x], axis=0)
                coarse = slope.astype(BF16)
                ghi[c, at, x * lanes : (x + 1) * lanes] = coarse
                glo[c, at, x * lanes : (x + 1) * lanes] = (slope - coarse.astype(F32)).astype(BF16)

    def slopes_of(whole, xr, yr, result, first=0, last=sensors):
        def step(i, carry):
            for k in range(UNROLL // 2):
                slope_pass(whole, xr, yr, result, UNROLL // 2 * i + k)
            return carry

        lax.fori_loop(first // UNROLL, last // UNROLL, step, 0)

    def gather(line):
        parts = []
        for c in range(3):
            product = jnp.dot(ghi[c], onehot[...], preferred_element_type=F32) + jnp.dot(
                glo[c], onehot[...], preferred_element_type=F32
            )
            for h in range(total_slots // lanes):
                raw[h] = product[:, h * lanes : (h + 1) * lanes]
            for g in range(sensors // 8):
                halves = []
                for h in range(total_slots // lanes):
                    acc = None
                    for y in range(cy):
                        strip = raw[h, pl.ds(8 * cy * g + y, 8, stride=cy), :]
                        term = jnp.where(y_of[:, h * lanes : (h + 1) * lanes] == y, strip, 0.0)
                        acc = term if acc is None else acc + term
                    halves.append(acc)
                parts.append(jnp.concatenate(halves, axis=1))
        parts.append(jnp.zeros((lanes - 3 * sensors, total_slots), F32))
        line[...] = jnp.concatenate(parts, axis=0).T

    def spread(source, target, axis):
        rows = source.shape[0] // count[axis]
        mine = pl.ds(pl.multiple_of(me[axis] * rows, rows), rows)
        copies = []
        for d in farthest_first(count[axis]):
            partner = lax.rem(me[axis] + d, count[axis])
            theirs = pl.ds(pl.multiple_of(partner * rows, rows), rows)
            copies.append((source.at[theirs, :], target.at[mine, :], {axis: partner}))
        arrived = ex.start(copies, target.at[pl.ds(0, rows * (count[axis] - 1)), :])
        target[mine, :] = source[mine, :]
        return [arrived]

    def spread_slabs(source, target, axis):
        mine = me[axis]
        copies = []
        for d in farthest_first(count[axis]):
            partner = lax.rem(mine + d, count[axis])
            copies.append((source.at[partner], target.at[mine], {axis: partner}))
        arrived = ex.start(copies, target.at[pl.ds(0, count[axis] - 1)])
        target[mine] = source[mine]
        return [arrived]

    tail = lane >= 3 * sensors
    first_rows = row < 4

    def regroup(mid, out):
        for iy in range(ny):
            rows = jnp.concatenate(
                [mid[pl.ds(iy * cap + t, nx, stride=ny * cap), :] for t in range(cap)], axis=0
            )
            for g in range(nx * cap // 16):
                a, b = rows[16 * g : 16 * g + 8, :], rows[16 * g + 8 : 16 * g + 16, :]
                p0 = pltpu.roll(pltpu.roll(b, lanes - sensors, 1), 4, 0)
                p1 = pltpu.roll(b, lanes - 2 * sensors, 1)
                p2 = pltpu.roll(pltpu.roll(b, lanes - 3 * sensors, 1), 4, 0)
                out[iy, 12 * g : 12 * g + 8, :] = jnp.where(tail, jnp.where(first_rows, p0, p1), a)
                out[iy, 12 * g + 8 : 12 * g + 12, :] = jnp.where(tail, p2, b)[0:4, :]

    def unpack(slabs):
        parts = []
        third = lane // sensors
        for iy in range(ny):
            for g in range(nx * cap // 16):
                a = slabs[iy, 12 * g : 12 * g + 8, :]
                b = jnp.concatenate([slabs[iy, 12 * g + 8 : 12 * g + 12, :]] * 2, axis=0)
                p0 = pltpu.roll(pltpu.roll(a, sensors, 1), 4, 0)
                p1 = pltpu.roll(a, 2 * sensors, 1)
                p2 = pltpu.roll(b, 3 * sensors, 1)
                last = jnp.where(third == 0, p0, jnp.where(third == 1, p1, p2))
                parts += [a, jnp.where(first_rows, b, last)]
        return jnp.concatenate(parts, axis=0)

    def reduce_start(buffer, value, partners):
        buffer[0] = value
        copies = [(buffer.at[0], buffer.at[k + 1], where) for k, where in enumerate(partners)]
        return ex.start(copies, buffer.at[pl.ds(1, len(partners))])

    def reduce_end(buffer, arrived):
        arrived.wait()
        value = buffer[0]
        for d in range(1, buffer.shape[0]):
            value = value + buffer[d]
        return value

    def moment_rows(m):
        parts = []
        for g in range(sensors // 8):
            acc = None
            for y in range(cy):
                strip = mq[m, pl.ds(8 * cy * g + y, 8, stride=cy), :]
                acc = strip if acc is None else acc + strip
            parts.append(acc)
        return parts

    def lane_sums(parts):
        return lax.dot_general(
            jnp.ones((8, lanes), F32),
            jnp.concatenate(parts, axis=0),
            (((1,), (1,)), ((), ())),
            precision=lax.Precision.HIGHEST,
            preferred_element_type=F32,
        )[0:1, :]

    def select(rows, pick):
        columns = rows.T
        coarse = columns.astype(BF16)
        fine = (columns - coarse.astype(F32)).astype(BF16)
        return jnp.dot(coarse, pick[...], preferred_element_type=F32) + jnp.dot(
            fine, pick[...], preferred_element_type=F32
        )

    def wait(copies):
        for copy in copies:
            copy.wait()

    blank = [jnp.zeros((8, lanes), F32)]
    steps_per_chunk = per_chunk // UNROLL
    wait(first_z)
    merge_z(zr_b)
    acc = no_z
    second = []
    for h in range(CHUNKS):
        wait(first_x[h] + first_y[h])
        acc = lax.fori_loop(steps_per_chunk * h, steps_per_chunk * (h + 1), image_pass, acc)
        second.append(x_faces(image, xr_v, h) + y_faces(ys_v, yr_v, h))
    store_z(zs_v, acc)
    second_z = z_faces(zs_v, zr_v)
    wave()
    slopes_of(field, xr_b, yr_b, image)
    early = lane_sums(moment_rows(0) + moment_rows(1) + moment_rows(2) + blank * (sensors // 8))
    gather(line_b)
    regroup(line_b, out_b)
    wave(len(plan))
    out_b_copies = spread_slabs(out_b, fin_b, "gy")
    wait(second_z)
    merge_z(zr_v)
    for h in range(CHUNKS):
        wait(second[h])
        slopes_of(image, xr_v, yr_v, None, per_chunk * h, per_chunk * (h + 1))
    partial = early + lane_sums(blank * (3 * sensors // 8) + moment_rows(3))
    plane = [
        {"gx": lax.rem(me["gx"] + dx, nx), "gz": lax.rem(me["gz"] + dz, nz)}
        for dx in farthest_first(nx) + [0]
        for dz in farthest_first(nz) + [0]
        if dx or dz
    ]
    plane_copies = reduce_start(red_plane, partial, plane)
    gather(line_v)
    line_v_copies = spread(line_v, mid_v, "gx")
    line = [{"gy": lax.rem(me["gy"] + d, ny)} for d in farthest_first(ny)]
    line_copies = reduce_start(red_line, reduce_end(red_plane, plane_copies), line)
    wait(line_v_copies)
    regroup(mid_v, out_v)
    out_v_copies = spread_slabs(out_v, fin_v, "gy")
    wait(out_b_copies)
    mid_b[...] = unpack(fin_b)
    for ix in range(nx):
        turn_b[ix * ny * cap : (ix + 1) * ny * cap, :] = mid_b[pl.ds(ix, ny * cap, stride=nx), :]
    last_b_copies = spread(turn_b, last_b, "gx")
    wait(last_b_copies)
    owned_b_out[...] = select(last_b[...], pick_b)
    wait(out_v_copies)
    owned_v_out[...] = select(unpack(fin_v), pick_v)
    moments_out[...] = jnp.broadcast_to(reduce_end(red_line, line_copies), (8, lanes))


def finish(moments_in, owned_b, owned_v, data, proj, gram):
    sensors = data.shape[0]
    moments = moments_in[...]
    lanes = moments.shape[1]
    group = lax.broadcasted_iota(jnp.int32, moments.shape, 1) // sensors
    full = []
    for m in range(4):
        value = moments
        for g in range(lanes // sensors):
            shift = (sensors * (g - m)) % lanes
            turn = pltpu.roll(moments, shift, 1) if shift else moments
            value = jnp.where(group == g, turn, value)
        full.append(value)
    zero, one, two, three = full
    first_step = zero / one
    residue = first_step * first_step * two - zero
    growth = 1.0 + residue / zero
    curvature = growth * growth * one - 2.0 * growth * first_step * two + first_step * first_step * three
    second_step = residue / curvature
    source_coef = (first_step + second_step * growth)[0:1, :]
    image_coef = (second_step * first_step)[0:1, :]
    down = (lanes, lanes)
    owned = jnp.broadcast_to(source_coef, down).T * owned_b[...] - jnp.broadcast_to(image_coef, down).T * owned_v[...]
    per_time = data[...].T
    parts = [owned[sensors * c : sensors * (c + 1), :] for c in range(3)]
    for c in range(3):
        proj[c] = jnp.dot(
            per_time, parts[c], precision=lax.Precision.HIGHEST, preferred_element_type=F32
        )
    for k, (a, b) in enumerate(PAIRS):
        gram[k : k + 1, :] = jnp.sum(parts[a] * parts[b], axis=0, keepdims=True)


def per_device(sizes, source_term, labels, table, send_map, owner_slots, sensor_data):
    sensors, cx, cy, lanes = source_term.shape
    cells_xy = cx * cy
    total = send_map.shape[-1]
    owned = owner_slots.shape[0]
    times = sensor_data.shape[1]
    vmem = pltpu.VMEM
    scratch = [
        vmem((cells_xy, lanes), jnp.int32),
        pltpu.SMEM(table.shape, F32),
        vmem((1, total), jnp.int32),
        vmem((1, owned), jnp.int32),
        vmem((sensors, cells_xy, lanes), F32),
        vmem((sensors, cells_xy, lanes), F32),
        vmem((2, sensors, 8, lanes), F32),
        vmem((2, sensors, 8, lanes), F32),
        vmem((2, sensors * cx, lanes), F32),
        vmem((2, sensors * cx, lanes), F32),
        vmem((2, sensors * cx, lanes), F32),
        vmem((2, sensors * cx, lanes), F32),
        vmem((cells_xy, lanes), F32),
        vmem((cells_xy, lanes), F32),
        vmem((2, cells_xy, lanes), F32),
        vmem((2, cells_xy, lanes), F32),
        vmem((cells_xy, lanes), F32),
        vmem((2 * cx, lanes), jnp.int32),
        vmem((2, 8, lanes), jnp.int32),
        vmem((2, 2 * cx, lanes), jnp.int32),
        vmem((2, cells_xy, lanes), jnp.int32),
        vmem((8, cells_xy, lanes), F32),
        vmem((3, sensors * 8, cx * lanes), BF16),
        vmem((3, sensors * 8, cx * lanes), BF16),
        vmem((cx * lanes, total), BF16),
        vmem((total, owned), BF16),
        vmem((total, owned), BF16),
        vmem((total // lanes, sensors * 8, lanes), F32),
    ]
    slabs = (sizes[1], total // sizes[1] * 3 // 4, lanes)
    scratch += [vmem((total, lanes), F32)] * 6
    scratch += [vmem(slabs, F32)] * 4
    scratch += [
        vmem((4, sensors * 8, lanes), F32),
        vmem((sizes[0] * sizes[2], 1, lanes), F32),
        vmem((sizes[1], 1, lanes), F32),
        pltpu.SemaphoreType.DMA((4 + CHUNKS,)),
        pltpu.SemaphoreType.DMA((GROUPS,)),
        pltpu.SemaphoreType.DMA((GROUPS,)),
        pltpu.SemaphoreType.REGULAR((len(AXES) * len(wave_plan(sizes)),)),
    ]
    whole = pl.BlockSpec(memory_space=pltpu.VMEM)
    moments, owned_b, owned_v = pl.pallas_call(
        functools.partial(kernel, sizes),
        out_shape=(
            jax.ShapeDtypeStruct((8, lanes), F32),
            jax.ShapeDtypeStruct((lanes, owned), F32),
            jax.ShapeDtypeStruct((lanes, owned), F32),
        ),
        in_specs=[pl.BlockSpec(memory_space=pltpu.HBM)] * 5,
        out_specs=(whole,) * 3,
        scratch_shapes=scratch,
        compiler_params=pltpu.CompilerParams(
            collective_id=0, has_side_effects=True, vmem_limit_bytes=40 * 1024 * 1024
        ),
        name="solve",
    )(
        *(
            pltpu.with_memory_space_constraint(operand, pltpu.HBM)
            for operand in (
                source_term.reshape(sensors, cells_xy, lanes),
                labels.reshape(cells_xy, lanes),
                table,
                send_map.reshape(1, total),
                owner_slots.reshape(1, owned),
            )
        )
    )
    return pl.pallas_call(
        finish,
        out_shape=(
            jax.ShapeDtypeStruct((3, times, owned), F32),
            jax.ShapeDtypeStruct((len(PAIRS), owned), F32),
        ),
        in_specs=[whole] * 4,
        out_specs=(whole, whole),
        compiler_params=pltpu.CompilerParams(vmem_limit_bytes=40 * 1024 * 1024),
        name="finish",
    )(moments, owned_b, owned_v, sensor_data)


def solution(mesh):
    sizes = tuple(mesh.shape[axis] for axis in AXES)
    in_specs = (
        P(None, "gx", "gy", "gz"),
        P("gx", "gy", "gz"),
        P(),
        P("gx", "gy", "gz", None),
        P(AXES),
        P(),
    )
    out_specs = (P(None, None, AXES), P(None, AXES))
    return jax.shard_map(
        functools.partial(per_device, sizes),
        mesh=mesh,
        in_specs=in_specs,
        out_specs=out_specs,
        check_vma=False,
    )
```

```python
import functools

import jax
import jax.numpy as jnp
from jax import lax
from jax.experimental import pallas as pl
from jax.experimental.pallas import tpu as pltpu
from jax.sharding import PartitionSpec as P

F32 = jnp.float32
BF16 = jnp.bfloat16
MASS = 0.25
PAIRS = ((0, 0), (1, 1), (2, 2), (0, 1), (0, 2), (1, 2))
AXES = ("gx", "gy", "gz")


class Exchange:
    def __init__(self, send, recv):
        self.send, self.recv, self.used = send, recv, 0

    def copy(self, source, target, where):
        return pltpu.make_async_remote_copy(
            src_ref=source,
            dst_ref=target,
            send_sem=self.send.at[self.used],
            recv_sem=self.recv.at[self.used],
            device_id=where,
            device_id_type=pl.DeviceIdType.MESH,
        )

    def start(self, copies, arrived):
        for source, target, where in copies:
            self.copy(source, target, where).start()
        whole = self.copy(arrived, arrived, copies[0][2])
        self.used += 1
        return whole


CHUNKS = 2
UNROLL = 16


GROUPS = 3 + 2 * (2 * CHUNKS + 1) + 4 + 2


def farthest_first(size):
    return sorted(range(1, size), key=lambda d: -min(d, size - d))


def doubling(known, size):
    strides = []
    while known < size // 2:
        strides.append(max(known, 1))
        known += strides[-1]
    return strides


def wave_plan(sizes):
    nx, ny, nz = sizes
    across = [("gx", d) for d in doubling(1, nx)] + [("gz", d) for d in doubling(0, nz)]
    along = [("gy", d) for d in doubling(1, ny)]
    plan = [[] for _ in range(max(len(across), len(along)))]
    for steps in (across, along):
        for k, step in enumerate(steps):
            plan[k].append(step)
    return plan


def kernel(sizes, src, lab_in, table_in, send_in, slots_in, moments_out, owned_b_out, owned_v_out,
           lab, table, send_map, slots, field, image, xr_b, xr_v, ys_b, ys_v, yr_b, yr_v,
           zs_b, zs_v, zr_b, zr_v, zm, lys, lxr, lyr, lzr, wts, ghi, glo, onehot, pick_b, pick_v, raw,
           line_b, line_v, mid_b, mid_v, turn_b, last_b, out_b, out_v, fin_b, fin_v, mq, red_plane, red_line,
           load_sem, send_sem, recv_sem, wave_sem):
    nx, ny, nz = sizes
    count = dict(zip(AXES, sizes))
    me = {axis: lax.axis_index(axis) for axis in AXES}
    low = {axis: lax.rem(me[axis] + count[axis] - 1, count[axis]) for axis in AXES}
    high = {axis: lax.rem(me[axis] + 1, count[axis]) for axis in AXES}
    has_low = {axis: me[axis] > 0 for axis in AXES}
    has_high = {axis: me[axis] < count[axis] - 1 for axis in AXES}
    keep_low = {axis: jnp.where(has_low[axis], 1.0, 0.0).astype(F32) for axis in AXES}
    keep_high = {axis: jnp.where(has_high[axis], 1.0, 0.0).astype(F32) for axis in AXES}
    sensors, cells_xy, lanes = field.shape
    cx, cy = cells_xy // 8, 8
    total_slots = send_map.shape[1]
    cap = total_slots // (nx * ny)
    per_chunk = sensors // CHUNKS
    ex = Exchange(send_sem, recv_sem)
    lane = lax.broadcasted_iota(jnp.int32, (8, lanes), 1)
    row = lax.broadcasted_iota(jnp.int32, (8, lanes), 0)

    def tell(sem, axis, partner):
        pl.semaphore_signal(
            sem, inc=1, device_id={axis: partner}, device_id_type=pl.DeviceIdType.MESH
        )

    loads = [pltpu.make_async_copy(lab_in, lab, load_sem.at[0])]
    for h in range(CHUNKS):
        part = pl.ds(per_chunk * h, per_chunk)
        loads.append(pltpu.make_async_copy(src.at[part], field.at[part], load_sem.at[1 + h]))
    for k, (a, b) in enumerate(((table_in, table), (send_in, send_map), (slots_in, slots))):
        loads.append(pltpu.make_async_copy(a, b, load_sem.at[1 + CHUNKS + k]))
    for copy in loads:
        copy.start()
    barrier = pltpu.get_barrier_semaphore()
    for axis in AXES:
        tell(barrier, axis, low[axis])
        tell(barrier, axis, high[axis])

    plan = wave_plan(sizes)
    wave_at = [0]

    def wave_sems(k, axis):
        before = sum(len(steps) for steps in plan[:k])
        return wave_sem.at[before + [step[0] for step in plan[k]].index(axis)]

    def wave_send():
        k = wave_at[0]
        if k < len(plan):
            for axis, stride in plan[k]:
                sem = wave_sems(k, axis)
                tell(sem, axis, lax.rem(me[axis] + count[axis] - stride, count[axis]))
                tell(sem, axis, lax.rem(me[axis] + stride, count[axis]))

    def wave(times=1):
        for _ in range(times):
            k = wave_at[0]
            if k < len(plan):
                for axis, _stride in plan[k]:
                    pl.semaphore_wait(wave_sems(k, axis), 2)
                wave_at[0] += 1
                wave_send()

    def both_ways(to_low, to_high, target, arrived, axis):
        copies = (
            (to_low, target(1), {axis: low[axis]}),
            (to_high, target(0), {axis: high[axis]}),
        )
        return [ex.start(copies, arrived)]

    def x_faces(whole, xr, h):
        part = pl.ds(per_chunk * h, per_chunk)
        last = cells_xy - 8
        return both_ways(
            whole.at[part, 0:8, :],
            whole.at[part, last : last + 8, :],
            lambda side: xr.at[side, part],
            xr.at[:, part],
            "gx",
        )

    def y_faces(ys, yr, h):
        part = pl.ds(per_chunk * h * cx, per_chunk * cx)
        return both_ways(
            ys.at[0, part], ys.at[1, part], lambda side: yr.at[side, part], yr.at[:, part], "gy"
        )

    def z_faces(zs, zr):
        return both_ways(zs, zs, lambda side: zr.at[side], zr, "gz")

    def pack_z(values, s, acc):
        here = lax.shift_right_logical(lane, 1) == s
        return tuple(
            jnp.where(here, pltpu.roll(values[x], 2 * s + 1, 1), acc[x]) for x in range(cx)
        )

    def store_z(zs, acc):
        for x in range(cx):
            zs[8 * x : 8 * x + 8, :] = acc[x]

    no_z = (jnp.zeros((8, lanes), F32),) * cx

    loads[0].wait()
    lys[0:cx, :] = lab[pl.ds(0, cx, stride=cy), :]
    lys[cx : 2 * cx, :] = lab[pl.ds(cy - 1, cx, stride=cy), :]
    pl.semaphore_wait(barrier, 2 * len(AXES))
    label_copies = (
        both_ways(lab.at[0:8, :], lab.at[cells_xy - 8 : cells_xy, :], lambda side: lxr.at[side], lxr, "gx")
        + both_ways(lys, lys, lambda side: lyr.at[side], lyr, "gy")
        + both_ways(lab, lab, lambda side: lzr.at[side], lzr, "gz")
    )
    wave_send()
    first_x = []
    for h in range(CHUNKS):
        loads[1 + h].wait()
        first_x.append(x_faces(field, xr_b, h))
    first_y = []
    for h in range(CHUNKS):
        for s in range(per_chunk * h, per_chunk * (h + 1)):
            for side, y in enumerate((0, cy - 1)):
                ys_b[side, cx * s : cx * s + cx, :] = field[s, pl.ds(y, cx, stride=cy), :]
        first_y.append(y_faces(ys_b, yr_b, h))
    store_z(
        zs_b,
        lax.fori_loop(
            0,
            sensors,
            lambda s, acc: pack_z([field[s, 8 * x : 8 * x + 8, :] for x in range(cx)], s, acc),
            no_z,
            unroll=32,
        ),
    )
    first_z = z_faces(zs_b, zr_b)

    for copy in loads[1 + CHUNKS :]:
        copy.wait()

    wanted = send_map[...]
    key = lax.shift_right_arithmetic(wanted, 10) * lanes + (wanted & (lanes - 1))
    y_of = lax.shift_right_arithmetic(wanted, 7) & (cy - 1)
    for x in range(cx):
        places = lax.broadcasted_iota(jnp.int32, (lanes, total_slots), 0) + x * lanes
        onehot[x * lanes : (x + 1) * lanes, :] = jnp.where(places == key, 1.0, 0.0).astype(BF16)
    rows_in = lax.broadcasted_iota(jnp.int32, (total_slots, slots.shape[1]), 0)
    slot_cap, slot_y = slots[...] % cap, slots[...] // cap % ny
    slot_row = slot_y * (nx * cap) + slot_cap * nx + slots[...] // (cap * ny)
    pick_v[...] = jnp.where(rows_in == slot_row, 1.0, 0.0).astype(BF16)
    pick_b[...] = jnp.where(rows_in == slots[...], 1.0, 0.0).astype(BF16)
    wave()

    for copy in label_copies:
        copy.wait()

    def tissue(shifted):
        level = jnp.zeros(shifted.shape, F32)
        for k in range(table.shape[0]):
            level = level + jnp.where(shifted == k + 1, table[k], 0.0)
        return level, jnp.where(shifted > 0, 1.0, 0.0).astype(F32)

    shifted = [lab[8 * x : 8 * x + 8, :] + 1 for x in range(cx)]
    for x in range(cx):
        here = shifted[x]
        if x > 0:
            x_low = shifted[x - 1]
        else:
            x_low = jnp.where(has_low["gx"], lxr[0] + 1, 0)
        if x < cx - 1:
            x_high = shifted[x + 1]
        else:
            x_high = jnp.where(has_high["gx"], lxr[1] + 1, 0)
        row_low = jnp.where(has_low["gy"], lyr[0, cx + x : cx + x + 1, :] + 1, 0)
        row_high = jnp.where(has_high["gy"], lyr[1, x : x + 1, :] + 1, 0)
        y_low = jnp.where(row == 0, row_low, pltpu.roll(here, 1, 0))
        y_high = jnp.where(row == cy - 1, row_high, pltpu.roll(here, cy - 1, 0))
        side_low = jnp.where(has_low["gz"], lzr[0, 8 * x : 8 * x + 8, :] + 1, 0)
        side_high = jnp.where(has_high["gz"], lzr[1, 8 * x : 8 * x + 8, :] + 1, 0)
        z_low = pltpu.roll(jnp.where(lane == lanes - 1, side_low, here), 1, 1)
        z_high = pltpu.roll(jnp.where(lane == 0, side_high, here), lanes - 1, 1)
        own_cond, own_in = tissue(here)
        diagonal = jnp.full((8, lanes), MASS, F32)
        for k, beside in enumerate((x_low, x_high, y_low, y_high, z_low, z_high)):
            its_cond, its_in = tissue(beside)
            weight = 0.5 * (own_cond + its_cond) * own_in * its_in
            wts[k, 8 * x : 8 * x + 8, :] = weight
            diagonal = diagonal + weight
        wts[6, 8 * x : 8 * x + 8, :] = diagonal
        wts[7, 8 * x : 8 * x + 8, :] = 0.5 * own_cond
    wave()

    def merge_z(zr):
        for x in range(cx):
            span = slice(8 * x, 8 * x + 8)
            zm[span, :] = jnp.where(
                (lane & 1) == 0,
                pltpu.roll(zr[0, span, :], 2, 1) * keep_low["gz"],
                zr[1, span, :] * keep_high["gz"],
            )

    def neighbours(whole, xr, yr, s, masked):
        own = [whole[s, 8 * x : 8 * x + 8, :] for x in range(cx)]
        outer = [xr[0, s]] + own + [xr[1, s]]
        if masked:
            outer[0], outer[-1] = outer[0] * keep_low["gx"], outer[-1] * keep_high["gx"]
        near = []
        for x in range(cx):
            u = own[x]
            low_row = yr[0, pl.ds(s * cx + x, 1), :]
            high_row = yr[1, pl.ds(s * cx + x, 1), :]
            if masked:
                low_row, high_row = low_row * keep_low["gy"], high_row * keep_high["gy"]
            y_low = jnp.where(row == 0, low_row, pltpu.roll(u, 1, 0))
            y_high = jnp.where(row == cy - 1, high_row, pltpu.roll(u, cy - 1, 0))
            beyond = pltpu.roll(zm[8 * x : 8 * x + 8, :], lanes - 2 - 2 * s, 1)
            z_low = jnp.where(lane == 0, beyond, pltpu.roll(u, 1, 1))
            z_high = jnp.where(lane == lanes - 1, beyond, pltpu.roll(u, lanes - 1, 1))
            near.append((outer[x], outer[x + 2], y_low, y_high, z_low, z_high))
        return own, near

    def apply(own, near, x):
        span = slice(8 * x, 8 * x + 8)
        q = wts[6, span, :] * own[x]
        for n in range(6):
            q = q - wts[n, span, :] * near[x][n]
        return q

    def rows_of(s):
        return pl.ds(pl.multiple_of(8 * s, 8), 8)

    def image_pass(i, acc):
        for k in range(UNROLL):
            s = UNROLL * i + k
            own, near = neighbours(field, xr_b, yr_b, s, False)
            results = [apply(own, near, x) for x in range(cx)]
            for x in range(cx):
                image[s, 8 * x : 8 * x + 8, :] = results[x]
                ys_v[0, pl.ds(s * cx + x, 1), :] = results[x][0:1, :]
                ys_v[1, pl.ds(s * cx + x, 1), :] = results[x][cy - 1 : cy, :]
            acc = pack_z(results, s, acc)
        return acc

    def slope_pass(whole, xr, yr, result, i):
        slopes = [[[None, None] for _ in range(cx)] for _ in range(3)]
        for k in range(2):
            s = 2 * i + k
            own, near = neighbours(whole, xr, yr, s, True)
            sums = [None, None, None]
            for x in range(cx):
                half = wts[7, 8 * x : 8 * x + 8, :]
                for c in range(3):
                    slopes[c][x][k] = half * (near[x][2 * c + 1] - near[x][2 * c])
                if result is not None:
                    q = result[s, 8 * x : 8 * x + 8, :]
                    for n, term in enumerate((own[x] * own[x], own[x] * q, q * q)):
                        sums[n] = term if sums[n] is None else sums[n] + term
                else:
                    term = own[x] * apply(own, near, x)
                    sums[0] = term if sums[0] is None else sums[0] + term
            if result is not None:
                for n in range(3):
                    mq[n, rows_of(s), :] = sums[n]
            else:
                mq[3, rows_of(s), :] = sums[0]
        at = pl.ds(pl.multiple_of(16 * i, 16), 16)
        for c in range(3):
            for x in range(cx):
                slope = jnp.concatenate(slopes[c][x], axis=0)
                coarse = slope.astype(BF16)
                ghi[c, at, x * lanes : (x + 1) * lanes] = coarse
                glo[c, at, x * lanes : (x + 1) * lanes] = (slope - coarse.astype(F32)).astype(BF16)

    def slopes_of(whole, xr, yr, result, first=0, last=sensors):
        def step(i, carry):
            for k in range(UNROLL // 2):
                slope_pass(whole, xr, yr, result, UNROLL // 2 * i + k)
            return carry

        lax.fori_loop(first // UNROLL, last // UNROLL, step, 0)

    def gather(line):
        parts = []
        for c in range(3):
            product = jnp.dot(ghi[c], onehot[...], preferred_element_type=F32) + jnp.dot(
                glo[c], onehot[...], preferred_element_type=F32
            )
            for h in range(total_slots // lanes):
                raw[h] = product[:, h * lanes : (h + 1) * lanes]
            for g in range(sensors // 8):
                halves = []
                for h in range(total_slots // lanes):
                    acc = None
                    for y in range(cy):
                        strip = raw[h, pl.ds(8 * cy * g + y, 8, stride=cy), :]
                        term = jnp.where(y_of[:, h * lanes : (h + 1) * lanes] == y, strip, 0.0)
                        acc = term if acc is None else acc + term
                    halves.append(acc)
                parts.append(jnp.concatenate(halves, axis=1))
        parts.append(jnp.zeros((lanes - 3 * sensors, total_slots), F32))
        line[...] = jnp.concatenate(parts, axis=0).T

    def spread(source, target, axis):
        rows = source.shape[0] // count[axis]
        mine = pl.ds(pl.multiple_of(me[axis] * rows, rows), rows)
        copies = []
        for d in farthest_first(count[axis]):
            partner = lax.rem(me[axis] + d, count[axis])
            theirs = pl.ds(pl.multiple_of(partner * rows, rows), rows)
            copies.append((source.at[theirs, :], target.at[mine, :], {axis: partner}))
        arrived = ex.start(copies, target.at[pl.ds(0, rows * (count[axis] - 1)), :])
        target[mine, :] = source[mine, :]
        return [arrived]

    def spread_slabs(source, target, axis):
        mine = me[axis]
        copies = []
        for d in farthest_first(count[axis]):
            partner = lax.rem(mine + d, count[axis])
            copies.append((source.at[partner], target.at[mine], {axis: partner}))
        arrived = ex.start(copies, target.at[pl.ds(0, count[axis] - 1)])
        target[mine] = source[mine]
        return [arrived]

    tail = lane >= 3 * sensors
    first_rows = row < 4

    def regroup(mid, out):
        for iy in range(ny):
            rows = jnp.concatenate(
                [mid[pl.ds(iy * cap + t, nx, stride=ny * cap), :] for t in range(cap)], axis=0
            )
            for g in range(nx * cap // 16):
                a, b = rows[16 * g : 16 * g + 8, :], rows[16 * g + 8 : 16 * g + 16, :]
                p0 = pltpu.roll(pltpu.roll(b, lanes - sensors, 1), 4, 0)
                p1 = pltpu.roll(b, lanes - 2 * sensors, 1)
                p2 = pltpu.roll(pltpu.roll(b, lanes - 3 * sensors, 1), 4, 0)
                out[iy, 12 * g : 12 * g + 8, :] = jnp.where(tail, jnp.where(first_rows, p0, p1), a)
                out[iy, 12 * g + 8 : 12 * g + 12, :] = jnp.where(tail, p2, b)[0:4, :]

    def unpack(slabs):
        parts = []
        third = lane // sensors
        for iy in range(ny):
            for g in range(nx * cap // 16):
                a = slabs[iy, 12 * g : 12 * g + 8, :]
                b = jnp.concatenate([slabs[iy, 12 * g + 8 : 12 * g + 12, :]] * 2, axis=0)
                p0 = pltpu.roll(pltpu.roll(a, sensors, 1), 4, 0)
                p1 = pltpu.roll(a, 2 * sensors, 1)
                p2 = pltpu.roll(b, 3 * sensors, 1)
                last = jnp.where(third == 0, p0, jnp.where(third == 1, p1, p2))
                parts += [a, jnp.where(first_rows, b, last)]
        return jnp.concatenate(parts, axis=0)

    def reduce_start(buffer, value, partners):
        buffer[0] = value
        copies = [(buffer.at[0], buffer.at[k + 1], where) for k, where in enumerate(partners)]
        return ex.start(copies, buffer.at[pl.ds(1, len(partners))])

    def reduce_end(buffer, arrived):
        arrived.wait()
        value = buffer[0]
        for d in range(1, buffer.shape[0]):
            value = value + buffer[d]
        return value

    def moment_rows(m):
        parts = []
        for g in range(sensors // 8):
            acc = None
            for y in range(cy):
                strip = mq[m, pl.ds(8 * cy * g + y, 8, stride=cy), :]
                acc = strip if acc is None else acc + strip
            parts.append(acc)
        return parts

    def lane_sums(parts):
        return lax.dot_general(
            jnp.ones((8, lanes), F32),
            jnp.concatenate(parts, axis=0),
            (((1,), (1,)), ((), ())),
            precision=lax.Precision.HIGHEST,
            preferred_element_type=F32,
        )[0:1, :]

    def select(rows, pick):
        columns = rows.T
        coarse = columns.astype(BF16)
        fine = (columns - coarse.astype(F32)).astype(BF16)
        return jnp.dot(coarse, pick[...], preferred_element_type=F32) + jnp.dot(
            fine, pick[...], preferred_element_type=F32
        )

    def wait(copies):
        for copy in copies:
            copy.wait()

    blank = [jnp.zeros((8, lanes), F32)]
    steps_per_chunk = per_chunk // UNROLL
    wait(first_z)
    merge_z(zr_b)
    acc = no_z
    second = []
    for h in range(CHUNKS):
        wait(first_x[h] + first_y[h])
        acc = lax.fori_loop(steps_per_chunk * h, steps_per_chunk * (h + 1), image_pass, acc)
        second.append(x_faces(image, xr_v, h) + y_faces(ys_v, yr_v, h))
    store_z(zs_v, acc)
    second_z = z_faces(zs_v, zr_v)
    wave()
    slopes_of(field, xr_b, yr_b, image)
    early = lane_sums(moment_rows(0) + moment_rows(1) + moment_rows(2) + blank * (sensors // 8))
    gather(line_b)
    regroup(line_b, out_b)
    wave(len(plan))
    out_b_copies = spread_slabs(out_b, fin_b, "gy")
    wait(second_z)
    merge_z(zr_v)
    for h in range(CHUNKS):
        wait(second[h])
        slopes_of(image, xr_v, yr_v, None, per_chunk * h, per_chunk * (h + 1))
    partial = early + lane_sums(blank * (3 * sensors // 8) + moment_rows(3))
    plane = [
        {"gx": lax.rem(me["gx"] + dx, nx), "gz": lax.rem(me["gz"] + dz, nz)}
        for dx in farthest_first(nx) + [0]
        for dz in farthest_first(nz) + [0]
        if dx or dz
    ]
    plane_copies = reduce_start(red_plane, partial, plane)
    gather(line_v)
    line_v_copies = spread(line_v, mid_v, "gx")
    line = [{"gy": lax.rem(me["gy"] + d, ny)} for d in farthest_first(ny)]
    line_copies = reduce_start(red_line, reduce_end(red_plane, plane_copies), line)
    wait(line_v_copies)
    regroup(mid_v, out_v)
    out_v_copies = spread_slabs(out_v, fin_v, "gy")
    wait(out_b_copies)
    mid_b[...] = unpack(fin_b)
    for ix in range(nx):
        turn_b[ix * ny * cap : (ix + 1) * ny * cap, :] = mid_b[pl.ds(ix, ny * cap, stride=nx), :]
    last_b_copies = spread(turn_b, last_b, "gx")
    wait(last_b_copies)
    owned_b_out[...] = select(last_b[...], pick_b)
    wait(out_v_copies)
    owned_v_out[...] = select(unpack(fin_v), pick_v)
    moments_out[...] = jnp.broadcast_to(reduce_end(red_line, line_copies), (8, lanes))


def finish(moments_in, owned_b, owned_v, data, proj, gram):
    sensors = data.shape[0]
    moments = moments_in[...]
    lanes = moments.shape[1]
    group = lax.broadcasted_iota(jnp.int32, moments.shape, 1) // sensors
    full = []
    for m in range(4):
        value = moments
        for g in range(lanes // sensors):
            shift = (sensors * (g - m)) % lanes
            turn = pltpu.roll(moments, shift, 1) if shift else moments
            value = jnp.where(group == g, turn, value)
        full.append(value)
    zero, one, two, three = full
    first_step = zero / one
    residue = first_step * first_step * two - zero
    growth = 1.0 + residue / zero
    curvature = growth * growth * one - 2.0 * growth * first_step * two + first_step * first_step * three
    second_step = residue / curvature
    source_coef = (first_step + second_step * growth)[0:1, :]
    image_coef = (second_step * first_step)[0:1, :]
    down = (lanes, lanes)
    owned = jnp.broadcast_to(source_coef, down).T * owned_b[...] - jnp.broadcast_to(image_coef, down).T * owned_v[...]
    per_time = data[...].T
    parts = [owned[sensors * c : sensors * (c + 1), :] for c in range(3)]
    for c in range(3):
        proj[c] = jnp.dot(
            per_time, parts[c], precision=lax.Precision.HIGHEST, preferred_element_type=F32
        )
    for k, (a, b) in enumerate(PAIRS):
        gram[k : k + 1, :] = jnp.sum(parts[a] * parts[b], axis=0, keepdims=True)


def per_device(sizes, source_term, labels, table, send_map, owner_slots, sensor_data):
    sensors, cx, cy, lanes = source_term.shape
    cells_xy = cx * cy
    total = send_map.shape[-1]
    owned = owner_slots.shape[0]
    times = sensor_data.shape[1]
    vmem = pltpu.VMEM
    scratch = [
        vmem((cells_xy, lanes), jnp.int32),
        pltpu.SMEM(table.shape, F32),
        vmem((1, total), jnp.int32),
        vmem((1, owned), jnp.int32),
        vmem((sensors, cells_xy, lanes), F32),
        vmem((sensors, cells_xy, lanes), F32),
        vmem((2, sensors, 8, lanes), F32),
        vmem((2, sensors, 8, lanes), F32),
        vmem((2, sensors * cx, lanes), F32),
        vmem((2, sensors * cx, lanes), F32),
        vmem((2, sensors * cx, lanes), F32),
        vmem((2, sensors * cx, lanes), F32),
        vmem((cells_xy, lanes), F32),
        vmem((cells_xy, lanes), F32),
        vmem((2, cells_xy, lanes), F32),
        vmem((2, cells_xy, lanes), F32),
        vmem((cells_xy, lanes), F32),
        vmem((2 * cx, lanes), jnp.int32),
        vmem((2, 8, lanes), jnp.int32),
        vmem((2, 2 * cx, lanes), jnp.int32),
        vmem((2, cells_xy, lanes), jnp.int32),
        vmem((8, cells_xy, lanes), F32),
        vmem((3, sensors * 8, cx * lanes), BF16),
        vmem((3, sensors * 8, cx * lanes), BF16),
        vmem((cx * lanes, total), BF16),
        vmem((total, owned), BF16),
        vmem((total, owned), BF16),
        vmem((total // lanes, sensors * 8, lanes), F32),
    ]
    slabs = (sizes[1], total // sizes[1] * 3 // 4, lanes)
    scratch += [vmem((total, lanes), F32)] * 6
    scratch += [vmem(slabs, F32)] * 4
    scratch += [
        vmem((4, sensors * 8, lanes), F32),
        vmem((sizes[0] * sizes[2], 1, lanes), F32),
        vmem((sizes[1], 1, lanes), F32),
        pltpu.SemaphoreType.DMA((4 + CHUNKS,)),
        pltpu.SemaphoreType.DMA((GROUPS,)),
        pltpu.SemaphoreType.DMA((GROUPS,)),
        pltpu.SemaphoreType.REGULAR((sum(len(steps) for steps in wave_plan(sizes)),)),
    ]
    whole = pl.BlockSpec(memory_space=pltpu.VMEM)
    moments, owned_b, owned_v = pl.pallas_call(
        functools.partial(kernel, sizes),
        out_shape=(
            jax.ShapeDtypeStruct((8, lanes), F32),
            jax.ShapeDtypeStruct((lanes, owned), F32),
            jax.ShapeDtypeStruct((lanes, owned), F32),
        ),
        in_specs=[pl.BlockSpec(memory_space=pltpu.HBM)] * 5,
        out_specs=(whole,) * 3,
        scratch_shapes=scratch,
        compiler_params=pltpu.CompilerParams(
            collective_id=0, has_side_effects=True, vmem_limit_bytes=40 * 1024 * 1024
        ),
        name="solve",
    )(
        *(
            pltpu.with_memory_space_constraint(operand, pltpu.HBM)
            for operand in (
                source_term.reshape(sensors, cells_xy, lanes),
                labels.reshape(cells_xy, lanes),
                table,
                send_map.reshape(1, total),
                owner_slots.reshape(1, owned),
            )
        )
    )
    return pl.pallas_call(
        finish,
        out_shape=(
            jax.ShapeDtypeStruct((3, times, owned), F32),
            jax.ShapeDtypeStruct((len(PAIRS), owned), F32),
        ),
        in_specs=[whole] * 4,
        out_specs=(whole, whole),
        compiler_params=pltpu.CompilerParams(vmem_limit_bytes=40 * 1024 * 1024),
        name="finish",
    )(moments, owned_b, owned_v, sensor_data)


def solution(mesh):
    sizes = tuple(mesh.shape[axis] for axis in AXES)
    in_specs = (
        P(None, "gx", "gy", "gz"),
        P("gx", "gy", "gz"),
        P(),
        P("gx", "gy", "gz", None),
        P(AXES),
        P(),
    )
    out_specs = (P(None, None, AXES), P(None, AXES))
    return jax.shard_map(
        functools.partial(per_device, sizes),
        mesh=mesh,
        in_specs=in_specs,
        out_specs=out_specs,
        check_vma=False,
    )
```
